128 devices in a mesh: xy: 8 (over z, core), gz: 4 (over y), ta: 4 (over x).
Axes of the slice: x: 4, y: 4, z: 4, core: 2. Of those that a mesh axis runs over, the one named last changes fastest.
Arguments:
- right_side: float32 [8, 4, 4, 128, 128], P('xy', 'gz', 'ta'), may hold values from -40 to 40
- link_blocks: float32 [8, 4, 4, 9, 2, 32, 32, 128], P('xy', 'gz', 'ta'), may hold values from -0.75 to 0.75
Outputs:
- solution: float32 [8, 4, 4, 128, 128], P('xy', 'gz', 'ta')
- residual: float32 [8, 4, 4, 128, 128], P('xy', 'gz', 'ta')
The draws below stay inside these ranges and needn't reach their ends.
All inputs are finite; a program needn't handle non-finite values.
Results may differ from the reference program's by a relative error of at most 0.00018.
Values sent between devices are 32-bit elements; how exact they have to be, the bound alone decides.
A program may use at most 128 MiB of HBM per device.

```python
import jax
import jax.numpy as jnp
from jax import lax

DOF = 32
RHS = 2
CX = 1
NY = 8
CZ = 2
CT = 8
ITERS = 2
S = 128
VEC = 128
NT = 32
N_XY = 8
N_GZ = 4
N_TA = 4


def draw_right_side(key, part):
    noise_key, rough_key = jax.random.split(jax.random.fold_in(key, 11), 2)
    shape = (N_XY, N_GZ, N_TA, S, VEC)
    time_index = (jnp.arange(N_TA)[:, None] * CT + jnp.arange(S)[None, :] % CT).astype(jnp.float32)
    ramp = jnp.exp(jnp.log(3.0) * time_index / max(NT - 1, 1))
    ramp = ramp[None, None, :, :, None]
    rough = jnp.exp(jax.random.uniform(rough_key, (N_XY, N_GZ, N_TA, S, 1), jnp.float32, -0.8, 0.8))
    base = jax.random.normal(noise_key, shape, jnp.float32)
    return jnp.clip(base * ramp * rough, -40.0, 40.0).astype(jnp.float32)


def steps_of(stream_key, dims, cuts, smallest, largest):
    gain = 1.0
    for position, shards_of in cuts:
        steps = jax.random.uniform(jax.random.fold_in(jax.random.fold_in(stream_key, 6), position), (shards_of,), jnp.float32, smallest / len(cuts), largest / len(cuts))
        gain = gain * jnp.repeat(jnp.exp(steps), dims[position] // shards_of).reshape((-1,) + (1,) * (len(dims) - 1 - position))
    return gain


def gaussian(stream_key, dims, spread, reach, shards=(), held_as=jnp.bfloat16):
    factor_of = steps_of(stream_key, dims, shards, -0.22, 0.18) if shards else 1.0
    drawn = jax.random.normal(stream_key, dims, jnp.float32) * spread * factor_of
    return jnp.minimum(jnp.maximum(drawn, -reach), reach).astype(held_as)


def setup_inputs(seed: int = 0) -> dict:
    arg_keys = jax.random.split(jax.random.key(seed), 3)
    right_side = draw_right_side(jax.random.fold_in(arg_keys[2], 71), 0)
    link_blocks = gaussian(arg_keys[1], (N_XY, N_GZ, N_TA, 9, 2, DOF, DOF, S), (2 * DOF) ** -0.5, 0.75, ((0, 8), (1, 4), (2, 4)), jnp.float32)
    return dict(right_side=right_side, link_blocks=link_blocks)


mass_shift = 4.0
epsilon = 1e-06

def split_parts(joined):
    shaped = joined.reshape(joined.shape[:-1] + (RHS, 2, DOF))
    return (shaped[..., 0, :], shaped[..., 1, :])

def join_parts(real, imaginary):
    stacked = jnp.stack((real, imaginary), -2)
    return stacked.reshape(stacked.shape[:-3] + (-1,))

def column_sums(values):
    folded = lax.optimization_barrier(jnp.sum(values, axis=-1))
    return lax.optimization_barrier(jnp.sum(folded.reshape(-1, folded.shape[-1]), axis=0))

def to_lattice(joined):
    shaped = joined.reshape(N_XY, N_GZ, N_TA, CX, NY, CZ, CT, joined.shape[-1])
    moved = jnp.transpose(shaped, (0, 3, 4, 1, 5, 2, 6, 7))
    return moved.reshape(N_XY * CX, NY, N_GZ * CZ, N_TA * CT, joined.shape[-1])

def to_blocks(lattice):
    shaped = lattice.reshape(N_XY, CX, NY, N_GZ, CZ, N_TA, CT, lattice.shape[-1])
    moved = jnp.transpose(shaped, (0, 3, 5, 1, 2, 4, 6, 7))
    return moved.reshape(N_XY, N_GZ, N_TA, CX * NY * CZ * CT, lattice.shape[-1])

def single(blocks, field):
    return jnp.einsum('...cds,...srd->...src', blocks, field, precision=lax.Precision.HIGHEST)

def apply_operator(link_blocks, real, imaginary):
    lattice = to_lattice(join_parts(real, imaginary))
    shifted_operator = [lattice]
    for axis_number in range(4):
        shifted_operator.append(jnp.roll(lattice, -1, axis_number))
        shifted_operator.append(jnp.roll(lattice, 1, axis_number))
    out_real = mass_shift * real
    output_imaginary = mass_shift * imaginary
    for level in range(9):
        near_real, near_imag = split_parts(to_blocks(shifted_operator[level]))
        blocks_real = link_blocks[:, :, :, level, 0]
        blocks_imag = link_blocks[:, :, :, level, 1]
        out_real = out_real + single(blocks_real, near_real) - single(blocks_imag, near_imag)
        output_imaginary = output_imaginary + single(blocks_real, near_imag) + single(blocks_imag, near_real)
    return (out_real, output_imaginary)

def solve_positive_definite(matrix, target):
    size = matrix.shape[0]
    lower = {}
    for row in range(size):
        for col in range(row + 1):
            value = matrix[row, col]
            for inner in range(col):
                value = value - lower[row, inner] * lower[col, inner]
            if row == col:
                lower[row, row] = jnp.sqrt(value)
            else:
                lower[row, col] = value / lower[col, col]
    forward = []
    for row in range(size):
        value = target[row]
        for inner in range(row):
            value = value - lower[row, inner] * forward[inner]
        forward.append(value / lower[row, row])
    answer = [None] * size
    for row in reversed(range(size)):
        value = forward[row]
        for inner in range(row + 1, size):
            value = value - lower[inner, row] * answer[inner]
        answer[row] = value / lower[row, row]
    return jnp.stack(answer)

def least_squares(hessenberg_real, hessenberg_imaginary, beta):
    exact_answer_vector = lax.Precision.HIGHEST
    gram_matrix_real = jnp.einsum('sxm,szm->xzm', hessenberg_real, hessenberg_real, precision=exact_answer_vector) + jnp.einsum('sxm,szm->xzm', hessenberg_imaginary, hessenberg_imaginary, precision=exact_answer_vector)
    gram_matrix_imaginary = jnp.einsum('sxm,szm->xzm', hessenberg_real, hessenberg_imaginary, precision=exact_answer_vector) - jnp.einsum('sxm,szm->xzm', hessenberg_imaginary, hessenberg_real, precision=exact_answer_vector)
    upper = jnp.concatenate((gram_matrix_real, -gram_matrix_imaginary), 1)
    bottom = jnp.concatenate((gram_matrix_imaginary, gram_matrix_real), 1)
    system = jnp.concatenate((upper, bottom), 0)
    target = jnp.concatenate((beta[None, :] * hessenberg_real[0], -beta[None, :] * hessenberg_imaginary[0]), 0)
    answer = solve_positive_definite(system, target)
    return (answer[:ITERS], answer[ITERS:])

def reference(right_side, link_blocks):
    rhs_real, rhs_imag = split_parts(right_side)
    beta = jnp.sqrt(column_sums(rhs_real * rhs_real + rhs_imag * rhs_imag) + epsilon)
    basis = [(rhs_real / beta[:, None], rhs_imag / beta[:, None])]
    hessenberg_real = jnp.zeros((ITERS + 1, ITERS, RHS), jnp.float32)
    hessenberg_imaginary = jnp.zeros((ITERS + 1, ITERS, RHS), jnp.float32)
    for step in range(ITERS):
        work_real, work_imag = apply_operator(link_blocks, basis[step][0], basis[step][1])
        proj_real = jnp.stack([column_sums(vector[0] * work_real + vector[1] * work_imag) for vector in basis])
        proj_imag = jnp.stack([column_sums(vector[0] * work_imag - vector[1] * work_real) for vector in basis])
        for index in range(len(basis)):
            coef_real = proj_real[index][:, None]
            coef_imag = proj_imag[index][:, None]
            vector = basis[index]
            work_real = work_real - (coef_real * vector[0] - coef_imag * vector[1])
            work_imag = work_imag - (coef_real * vector[1] + coef_imag * vector[0])
        norm = jnp.sqrt(column_sums(work_real * work_real + work_imag * work_imag) + epsilon)
        hessenberg_real = hessenberg_real.at[:step + 1, step].set(proj_real)
        hessenberg_imaginary = hessenberg_imaginary.at[:step + 1, step].set(proj_imag)
        hessenberg_real = hessenberg_real.at[step + 1, step].set(norm)
        basis.append((work_real / norm[:, None], work_imag / norm[:, None]))
    coef_real, coef_imag = least_squares(hessenberg_real, hessenberg_imaginary, beta)
    sol_real = jnp.zeros_like(rhs_real)
    sol_imag = jnp.zeros_like(rhs_imag)
    for index in range(ITERS):
        weight_real = coef_real[index][:, None]
        weight_imag = coef_imag[index][:, None]
        sol_real = sol_real + weight_real * basis[index][0] - weight_imag * basis[index][1]
        sol_imag = sol_imag + weight_real * basis[index][1] + weight_imag * basis[index][0]
    image_real, image_imag = apply_operator(link_blocks, sol_real, sol_imag)
    return (join_parts(sol_real, sol_imag), join_parts(rhs_real - image_real, rhs_imag - image_imag))
```

```python
import functools

import jax
import jax.numpy as jnp
from jax import lax
from jax.experimental import pallas as pl
from jax.experimental.pallas import tpu as pltpu
from jax.sharding import PartitionSpec as P

DOF = 32
RHS = 2
SITES = 128
VEC = 128
AXES = ("xy", "gz", "ta")
MESH = pl.DeviceIdType.MESH

mass_shift = 4.0
epsilon = 1e-06

LOCAL = (0, 3, 4)
REMOTE = (1, 2, 5, 6, 7, 8)


def offsets_of(sizes):
    nx, nz, nt = sizes
    first = [(d, 0, 0) for d in range(1, nx)]
    second = [(0, a, b) for a in range(nz) for b in range(nt) if (a, b) != (0, 0)]
    return first, second


def turn(value, shift):
    return pltpu.roll(value, shift % SITES, 1)


def rows_of_sums(tiles, row):
    for half in (4, 2, 1):
        low = (row & half) == 0
        tiles = [
            jnp.where(low, tiles[i], pltpu.roll(tiles[i + half], half, 0))
            + jnp.where(low, pltpu.roll(tiles[i], 8 - half, 0), tiles[i + half])
            for i in range(half)
        ]
    return tiles[0]


def kernel(
    sizes,
    rhs_hbm,
    links_hbm,
    sol_ref,
    res_ref,
    links,
    start,
    field,
    near,
    partial,
    x_in,
    z_out,
    z_in,
    t_out,
    t_in,
    row_out,
    first_in,
    second_in,
    link_sem,
    start_sem,
    halo_send,
    halo_recv,
    first_send,
    first_recv,
    second_send,
    second_recv,
):
    here = [lax.axis_index(name) for name in AXES]
    first, second = offsets_of(sizes)

    def device(offset):
        return tuple(
            here[i] if offset[i] == 0 else lax.rem(here[i] + (offset[i] % sizes[i]), sizes[i])
            for i in range(3)
        )

    barrier = pltpu.get_barrier_semaphore()
    for offset in first + second:
        pl.semaphore_signal(barrier, inc=1, device_id=device(offset), device_id_type=MESH)
    load = pltpu.make_async_copy(rhs_hbm, start, start_sem)
    load.start()
    link_loads = {}
    for k in LOCAL + REMOTE:
        link_loads[k] = pltpu.make_async_copy(links_hbm.at[k], links.at[k], link_sem.at[k])
        link_loads[k].start()

    lane = lax.broadcasted_iota(jnp.int32, (8, SITES), 1)
    row = lax.broadcasted_iota(jnp.int32, (8, SITES), 0)
    lane_z = (lane // 8) % 2
    lane_t = lane % 8

    def wide(mask, rows):
        return jnp.tile(mask, (rows // 8, 1)) if rows > 8 else mask

    def put(k, value):
        for r in range(RHS):
            real = value[64 * r : 64 * r + 32]
            imag = value[64 * r + 32 : 64 * r + 64]
            near[k, r, 0] = real
            near[k, r, 1] = real + imag
            near[k, r, 2] = imag - real

    def remote(j, n, src, dst, offset):
        return pltpu.make_async_remote_copy(
            src_ref=src,
            dst_ref=dst,
            send_sem=halo_send.at[j, n],
            recv_sem=halo_recv.at[j, n],
            device_id=device(offset),
            device_id_type=MESH,
        )

    z_is = [wide(lane_z == p, 64) for p in range(2)]
    t_is = [wide(lane_t == p, 16) for p in range(8)]

    def pack(j, value):
        low, high = value[:64], value[64:]
        z_out[j, 0] = jnp.where(z_is[0], low, turn(high, 8))
        z_out[j, 1] = jnp.where(z_is[1], low, turn(high, -8))
        ahead = value[:16]
        behind = value[112:]
        for g in range(1, 8):
            ahead = jnp.where(t_is[g], turn(value[16 * g : 16 * g + 16], g), ahead)
        for g in range(7):
            behind = jnp.where(t_is[g], turn(value[16 * g : 16 * g + 16], g - 7), behind)
        t_out[j, 0] = ahead
        t_out[j, 1] = behind

    def send(j):
        copies = [
            remote(j, 0, field.at[j], x_in.at[j, 0], (-1, 0, 0)),
            remote(j, 1, field.at[j], x_in.at[j, 1], (1, 0, 0)),
            remote(j, 2, z_out.at[j, 0], z_in.at[j, 0], (0, -1, 0)),
            remote(j, 3, z_out.at[j, 1], z_in.at[j, 1], (0, 1, 0)),
            remote(j, 4, t_out.at[j, 0], t_in.at[j, 0], (0, 0, -1)),
            remote(j, 5, t_out.at[j, 1], t_in.at[j, 1], (0, 0, 1)),
        ]
        for copy in copies:
            copy.start()
        return copies

    def put_local(j):
        value = field[j]
        put(0, value)
        put(3, turn(value, -16))
        put(4, turn(value, 16))

    def put_remote(j):
        put(1, x_in[j, 0])
        put(2, x_in[j, 1])
        value = field[j]
        low, high = value[:64], value[64:]
        came = z_in[j, 0]
        put(
            5,
            jnp.concatenate(
                (
                    jnp.where(z_is[0], turn(low, -8), turn(came, 8)),
                    jnp.where(z_is[0], turn(high, -8), came),
                )
            ),
        )
        came = z_in[j, 1]
        put(
            6,
            jnp.concatenate(
                (
                    jnp.where(z_is[1], turn(low, 8), turn(came, -8)),
                    jnp.where(z_is[1], turn(high, 8), came),
                )
            ),
        )
        came = t_in[j, 0]
        put(
            7,
            jnp.concatenate(
                [
                    jnp.where(t_is[7], turn(came, 7 - g), turn(value[16 * g : 16 * g + 16], -1))
                    for g in range(8)
                ]
            ),
        )
        came = t_in[j, 1]
        put(
            8,
            jnp.concatenate(
                [
                    jnp.where(t_is[0], turn(came, -g), turn(value[16 * g : 16 * g + 16], 1))
                    for g in range(8)
                ]
            ),
        )

    def sweep(ks, target):
        def body(block, carry):
            done = [[] for _ in range(4)]
            for half in range(2):
                sites = [block * 8 + half * 4 + i for i in range(4)]
                if target is None:
                    sums = [[None] * 6 for _ in sites]
                else:
                    sums = [[partial[c, q] for q in range(6)] for c in sites]
                for k in ks:
                    for t in range(4):
                        rows = slice(8 * t, 8 * t + 8)
                        value = [near[k, r, q, rows, :] for r in range(RHS) for q in range(3)]
                        for i, c in enumerate(sites):
                            real = links[k, 0, c, rows, :]
                            imag = links[k, 1, c, rows, :]
                            factors = (real + imag, imag, real)
                            for q in range(6):
                                term = factors[q % 3] * value[q]
                                sums[i][q] = term if sums[i][q] is None else sums[i][q] + term
                for i, c in enumerate(sites):
                    if target is None:
                        for q in range(6):
                            partial[c, q] = sums[i][q]
                    else:
                        for r in range(RHS):
                            done[2 * r].append(sums[i][3 * r] - sums[i][3 * r + 1])
                            done[2 * r + 1].append(sums[i][3 * r] + sums[i][3 * r + 2])
            if target is not None:
                for n in range(4):
                    place = pl.multiple_of(32 * n + block * 8, 8)
                    field[target, pl.ds(place, 8), :] = rows_of_sums(done[n], row)
            return carry

        lax.fori_loop(0, 4, body, 0)

    def parts(j, r):
        return field[j, 64 * r : 64 * r + 32, :], field[j, 64 * r + 32 : 64 * r + 64, :]

    def folded(value):
        value = value[:8] + value[8:16] + value[16:24] + value[24:]
        return jnp.sum(value, axis=1, keepdims=True)

    def gram(pairs, packed):
        for n, i, j, kind in pairs:
            for r in range(RHS):
                ar, ai = parts(i, r)
                br, bi = (ar, ai) if i == j else parts(j, r)
                value = ar * br + ai * bi if kind == 0 else ar * bi - ai * br
                packed = jnp.where(lane == 2 * n + r, folded(value), packed)
        return packed

    load.wait()
    begin = start[...].T
    field[0] = begin
    pack(0, begin)
    pl.semaphore_wait(barrier, len(first) + len(second))
    halos = send(0)
    put_local(0)
    for k in LOCAL:
        link_loads[k].wait()
    sweep(LOCAL, None)
    for k in REMOTE:
        link_loads[k].wait()
    for copy in halos:
        copy.wait_recv()
    put_remote(0)
    sweep(REMOTE, 1)

    again = field[1]
    pack(1, again)
    later = send(1)
    put_local(1)
    sweep(LOCAL, None)
    packed = gram(
        ((0, 0, 0, 0), (1, 0, 1, 0), (2, 0, 1, 1), (3, 1, 1, 0)), jnp.zeros((8, SITES), jnp.float32)
    )
    for copy in later:
        copy.wait_recv()
    put_remote(1)
    sweep(REMOTE, 2)
    packed = gram(
        ((4, 0, 2, 0), (5, 0, 2, 1), (6, 1, 2, 0), (7, 1, 2, 1), (8, 2, 2, 0)), packed
    )

    def reduce_over(offsets, own, index, arrived, send_sem, recv_sem):
        row_out[index] = own
        copies = []
        for n, offset in enumerate(offsets):
            copies.append(
                pltpu.make_async_remote_copy(
                    src_ref=row_out.at[index],
                    dst_ref=arrived.at[n],
                    send_sem=send_sem.at[n],
                    recv_sem=recv_sem.at[n],
                    device_id=device(offset),
                    device_id_type=MESH,
                )
            )
            copies[-1].start()
        total = own
        for n, copy in enumerate(copies):
            copy.wait_recv()
            total = total + arrived[n]
        return total, copies

    own = jnp.sum(packed, axis=0, keepdims=True)
    own, sent_a = reduce_over(first, own, 0, first_in, first_send, first_recv)
    own, sent_b = reduce_over(second, own, 1, second_in, second_send, second_recv)

    spread = jnp.broadcast_to(own, (8, SITES))
    g = [
        jnp.broadcast_to(
            jnp.sum(
                jnp.where((lane == 2 * n + row) & (row < 2), spread, 0.0), axis=1, keepdims=True
            ),
            (8, SITES),
        )
        for n in range(9)
    ]
    g00, g01r, g01i, g11, g02r, g02i, g12r, g12i, g22 = g
    ib = 1.0 / (g00 + epsilon)
    kr = (g01r - mass_shift * epsilon) * ib
    ki = g01i * ib
    hr = kr + mass_shift
    hi = ki
    kk = kr * kr + ki * ki
    wp = (g11 - 2.0 * (kr * g01r + ki * g01i) + kk * g00) * ib
    n1 = wp + epsilon
    in1 = 1.0 / n1
    er = epsilon * hr * ib
    ei = epsilon * hi * ib
    tr = (g02r - (kr * g01r - ki * g01i)) * ib
    ti = (g02i - (kr * g01i + ki * g01r)) * ib
    sr = mass_shift * er + tr
    si = mass_shift * ei + ti
    both = ib * in1
    ur = (g12r - kr * g11 - (kr * g02r + ki * g02i) + kk * g01r) * both
    ui = (g12i - ki * g11 - (kr * g02i - ki * g02r) + kk * g01i) * both
    pr = ur - mass_shift * epsilon * in1
    pi = ui
    h11r = pr + mass_shift
    h11i = pi
    q2 = (g22 - 2.0 * (kr * g12r + ki * g12i) + kk * g11) * both
    cross = sr * (pr * er - pi * ei) + si * (pr * ei + pi * er)
    n2 = (
        q2
        + (sr * sr + si * si) * in1 * (g00 * ib)
        + (pr * pr + pi * pi) * (wp * in1)
        - 2.0 * (sr * tr + si * ti) * in1
        - 2.0 * (pr * ur + pi * ui)
        + 2.0 * cross * in1
        + epsilon
    )
    mr = hr * h11r - hi * h11i - sr
    mi = hr * h11i + hi * h11r - si
    idet = 1.0 / (mr * mr + mi * mi + n2 * (hr * hr + hi * hi + n1))
    x1r = -mr * idet
    x1i = mi * idet
    fr = h11r + kr
    fi = h11i + ki
    x0r = (fr * mr + fi * mi + hr * n2) * idet
    x0i = (fi * mr - fr * mi - hi * n2) * idet

    sol, res = [], []
    for r in range(RHS):
        c0r, c0i, c1r, c1i = (v[r : r + 1, :] for v in (x0r, x0i, x1r, x1i))
        d0r = 1.0 - mass_shift * c0r
        d0i = -mass_shift * c0i
        d1r = mass_shift * c1r + c0r
        d1i = mass_shift * c1i + c0i
        ar, ai = parts(0, r)
        br, bi = parts(1, r)
        cr, ci = parts(2, r)
        sol.append(c0r * ar - c0i * ai + c1r * br - c1i * bi)
        sol.append(c0r * ai + c0i * ar + c1r * bi + c1i * br)
        res.append(d0r * ar - d0i * ai - (d1r * br - d1i * bi) - (c1r * cr - c1i * ci))
        res.append(d0r * ai + d0i * ar - (d1r * bi + d1i * br) - (c1r * ci + c1i * cr))
    sol_ref[...] = jnp.concatenate(sol).T
    res_ref[...] = jnp.concatenate(res).T
    for copy in halos + later + sent_a + sent_b:
        copy.wait_send()


def shards(sizes, right_side, link_blocks):
    first, second = offsets_of(sizes)
    f32 = jnp.float32
    sol, res = pl.pallas_call(
        functools.partial(kernel, sizes),
        out_shape=(
            jax.ShapeDtypeStruct((SITES, VEC), f32),
            jax.ShapeDtypeStruct((SITES, VEC), f32),
        ),
        in_specs=[pl.BlockSpec(memory_space=pl.ANY)] * 2,
        out_specs=(pl.BlockSpec(memory_space=pltpu.VMEM),) * 2,
        scratch_shapes=[
            pltpu.VMEM((9, 2, DOF, DOF, SITES), f32),
            pltpu.VMEM((SITES, VEC), f32),
            pltpu.VMEM((3, VEC, SITES), f32),
            pltpu.VMEM((9, RHS, 3, DOF, SITES), f32),
            pltpu.VMEM((DOF, 6, 8, SITES), f32),
            pltpu.VMEM((2, 2, VEC, SITES), f32),
            pltpu.VMEM((2, 2, 64, SITES), f32),
            pltpu.VMEM((2, 2, 64, SITES), f32),
            pltpu.VMEM((2, 2, 16, SITES), f32),
            pltpu.VMEM((2, 2, 16, SITES), f32),
            pltpu.VMEM((2, 1, SITES), f32),
            pltpu.VMEM((len(first), 1, SITES), f32),
            pltpu.VMEM((len(second), 1, SITES), f32),
            pltpu.SemaphoreType.DMA((9,)),
            pltpu.SemaphoreType.DMA,
            pltpu.SemaphoreType.DMA((2, 6)),
            pltpu.SemaphoreType.DMA((2, 6)),
            pltpu.SemaphoreType.DMA((len(first),)),
            pltpu.SemaphoreType.DMA((len(first),)),
            pltpu.SemaphoreType.DMA((len(second),)),
            pltpu.SemaphoreType.DMA((len(second),)),
        ],
        compiler_params=pltpu.CompilerParams(
            collective_id=0, has_side_effects=True
        ),
    )(
        right_side.reshape(SITES, VEC),
        link_blocks.reshape(9, 2, DOF, DOF, SITES),
    )
    return sol.reshape(right_side.shape), res.reshape(right_side.shape)


def solution(mesh):
    sizes = tuple(mesh.shape[name] for name in AXES)
    spec = P("xy", "gz", "ta", None, None)
    return jax.shard_map(
        functools.partial(shards, sizes),
        mesh=mesh,
        in_specs=(spec, P("xy", "gz", "ta", None, None, None, None, None)),
        out_specs=(spec, spec),
        check_vma=False,
    )
```

```python
import functools

import jax
import jax.numpy as jnp
from jax import lax
from jax.experimental import pallas as pl
from jax.experimental.pallas import tpu as pltpu
from jax.sharding import PartitionSpec as P

DOF = 32
RHS = 2
SITES = 128
VEC = 128
AXES = ("xy", "gz", "ta")
MESH = pl.DeviceIdType.MESH

mass_shift = 4.0
epsilon = 1e-06

LOCAL = (0, 3, 4)
REMOTE = (1, 2, 5, 6, 7, 8)


def offsets_of(sizes):
    nx, nz, nt = sizes
    first = [(d, 0, 0) for d in range(1, nx)]
    second = [(0, a, b) for a in range(nz) for b in range(nt) if (a, b) != (0, 0)]

    def hops(offset):
        return sum(min(d, n - d) for d, n in zip(offset, sizes))

    beside = [offset for offset in first + second if hops(offset) == 1]
    further = [offset for offset in first + second if hops(offset) == 2]
    return first, second, beside, further


def turn(value, shift):
    return pltpu.roll(value, shift % SITES, 1)


def rows_of_sums(tiles, row):
    for half in (4, 2, 1):
        low = (row & half) == 0
        tiles = [
            jnp.where(low, tiles[i], pltpu.roll(tiles[i + half], half, 0))
            + jnp.where(low, pltpu.roll(tiles[i], 8 - half, 0), tiles[i + half])
            for i in range(half)
        ]
    return tiles[0]


def kernel(
    sizes,
    rhs_hbm,
    links_hbm,
    both_ref,
    links,
    start,
    field,
    near,
    partial,
    x_in,
    z_out,
    z_in,
    t_out,
    t_in,
    row_out,
    first_in,
    second_in,
    link_sem,
    start_sem,
    halo_send,
    halo_recv,
    first_send,
    first_recv,
    second_send,
    second_recv,
    ready,
):
    here = [lax.axis_index(name) for name in AXES]
    first, second, beside, further = offsets_of(sizes)

    def device(offset):
        return tuple(
            here[i] if offset[i] == 0 else lax.rem(here[i] + (offset[i] % sizes[i]), sizes[i])
            for i in range(3)
        )

    load = pltpu.make_async_copy(rhs_hbm, start, start_sem)
    load.start()
    barrier = pltpu.get_barrier_semaphore()
    for offset in beside:
        pl.semaphore_signal(barrier, inc=1, device_id=device(offset), device_id_type=MESH)
    link_loads = {}
    for k in LOCAL + REMOTE:
        link_loads[k] = pltpu.make_async_copy(links_hbm.at[k], links.at[k], link_sem.at[k])
        link_loads[k].start()

    lane = lax.broadcasted_iota(jnp.int32, (8, SITES), 1)
    row = lax.broadcasted_iota(jnp.int32, (8, SITES), 0)
    lane_z = (lane // 8) % 2
    lane_t = lane % 8

    def wide(mask, rows):
        return jnp.tile(mask, (rows // 8, 1)) if rows > 8 else mask

    def put(k, value):
        for r in range(RHS):
            real = value[64 * r : 64 * r + 32]
            imag = value[64 * r + 32 : 64 * r + 64]
            near[k, r, 0] = real
            near[k, r, 1] = real + imag
            near[k, r, 2] = imag - real

    def remote(j, n, src, dst, offset):
        return pltpu.make_async_remote_copy(
            src_ref=src,
            dst_ref=dst,
            send_sem=halo_send.at[j, n],
            recv_sem=halo_recv.at[j, n],
            device_id=device(offset),
            device_id_type=MESH,
        )

    z_is = [wide(lane_z == p, 64) for p in range(2)]
    t_is = [wide(lane_t == p, 16) for p in range(8)]

    def pack(j, value):
        low, high = value[:64], value[64:]
        z_out[j, 0] = jnp.where(z_is[0], low, turn(high, 8))
        z_out[j, 1] = jnp.where(z_is[1], low, turn(high, -8))
        ahead = value[:16]
        behind = value[112:]
        for g in range(1, 8):
            ahead = jnp.where(t_is[g], turn(value[16 * g : 16 * g + 16], g), ahead)
        for g in range(7):
            behind = jnp.where(t_is[g], turn(value[16 * g : 16 * g + 16], g - 7), behind)
        t_out[j, 0] = ahead
        t_out[j, 1] = behind

    def send(j):
        copies = [
            remote(j, 0, field.at[j], x_in.at[j, 0], (-1, 0, 0)),
            remote(j, 1, field.at[j], x_in.at[j, 1], (1, 0, 0)),
            remote(j, 2, z_out.at[j, 0], z_in.at[j, 0], (0, -1, 0)),
            remote(j, 3, z_out.at[j, 1], z_in.at[j, 1], (0, 1, 0)),
            remote(j, 4, t_out.at[j, 0], t_in.at[j, 0], (0, 0, -1)),
            remote(j, 5, t_out.at[j, 1], t_in.at[j, 1], (0, 0, 1)),
        ]
        for copy in copies:
            copy.start()
        return copies

    def put_local(j):
        value = field[j]
        put(0, value)
        put(3, turn(value, -16))
        put(4, turn(value, 16))

    def put_remote(j):
        put(1, x_in[j, 0])
        put(2, x_in[j, 1])
        value = field[j]
        low, high = value[:64], value[64:]
        came = z_in[j, 0]
        put(
            5,
            jnp.concatenate(
                (
                    jnp.where(z_is[0], turn(low, -8), turn(came, 8)),
                    jnp.where(z_is[0], turn(high, -8), came),
                )
            ),
        )
        came = z_in[j, 1]
        put(
            6,
            jnp.concatenate(
                (
                    jnp.where(z_is[1], turn(low, 8), turn(came, -8)),
                    jnp.where(z_is[1], turn(high, 8), came),
                )
            ),
        )
        came = t_in[j, 0]
        put(
            7,
            jnp.concatenate(
                [
                    jnp.where(t_is[7], turn(came, 7 - g), turn(value[16 * g : 16 * g + 16], -1))
                    for g in range(8)
                ]
            ),
        )
        came = t_in[j, 1]
        put(
            8,
            jnp.concatenate(
                [
                    jnp.where(t_is[0], turn(came, -g), turn(value[16 * g : 16 * g + 16], 1))
                    for g in range(8)
                ]
            ),
        )

    def sweep(ks, target):
        def body(block, carry):
            done = [[] for _ in range(4)]
            for half in range(2):
                sites = [block * 8 + half * 4 + i for i in range(4)]
                if target is None:
                    sums = [[None] * 6 for _ in sites]
                else:
                    sums = [[partial[c, q] for q in range(6)] for c in sites]
                for k in ks:
                    for t in range(4):
                        rows = slice(8 * t, 8 * t + 8)
                        value = [near[k, r, q, rows, :] for r in range(RHS) for q in range(3)]
                        for i, c in enumerate(sites):
                            real = links[k, 0, c, rows, :]
                            imag = links[k, 1, c, rows, :]
                            factors = (real + imag, imag, real)
                            for q in range(6):
                                term = factors[q % 3] * value[q]
                                sums[i][q] = term if sums[i][q] is None else sums[i][q] + term
                for i, c in enumerate(sites):
                    if target is None:
                        for q in range(6):
                            partial[c, q] = sums[i][q]
                    else:
                        for r in range(RHS):
                            done[2 * r].append(sums[i][3 * r] - sums[i][3 * r + 1])
                            done[2 * r + 1].append(sums[i][3 * r] + sums[i][3 * r + 2])
            if target is not None:
                for n in range(4):
                    place = pl.multiple_of(32 * n + block * 8, 8)
                    field[target, pl.ds(place, 8), :] = rows_of_sums(done[n], row)
            return carry

        lax.fori_loop(0, 4, body, 0)

    def parts(j, r):
        return field[j, 64 * r : 64 * r + 32, :], field[j, 64 * r + 32 : 64 * r + 64, :]

    def folded(value):
        value = value[:8] + value[8:16] + value[16:24] + value[24:]
        return jnp.sum(value, axis=1, keepdims=True)

    def gram(pairs, packed):
        for n, i, j, kind in pairs:
            for r in range(RHS):
                ar, ai = parts(i, r)
                br, bi = (ar, ai) if i == j else parts(j, r)
                value = ar * br + ai * bi if kind == 0 else ar * bi - ai * br
                packed = jnp.where(lane == 2 * n + r, folded(value), packed)
        return packed

    load.wait()
    begin = start[...].T
    field[0] = begin
    pack(0, begin)
    pl.semaphore_wait(barrier, len(beside))
    halos = send(0)
    put_local(0)
    for k in LOCAL:
        link_loads[k].wait()
    sweep(LOCAL, None)
    for k in REMOTE:
        link_loads[k].wait()
    for copy in halos:
        copy.wait_recv()
    for offset in further:
        pl.semaphore_signal(ready, inc=1, device_id=device(offset), device_id_type=MESH)
    put_remote(0)
    sweep(REMOTE, 1)

    again = field[1]
    pack(1, again)
    later = send(1)
    put_local(1)
    sweep(LOCAL, None)
    packed = gram(
        ((0, 0, 0, 0), (1, 0, 1, 0), (2, 0, 1, 1), (3, 1, 1, 0)), jnp.zeros((8, SITES), jnp.float32)
    )
    for copy in later:
        copy.wait_recv()
    put_remote(1)
    sweep(REMOTE, 2)
    packed = gram(
        ((4, 0, 2, 0), (5, 0, 2, 1), (6, 1, 2, 0), (7, 1, 2, 1), (8, 2, 2, 0)), packed
    )

    def reduce_over(offsets, own, index, arrived, send_sem, recv_sem):
        row_out[index] = own
        copies = []
        for n, offset in enumerate(offsets):
            copies.append(
                pltpu.make_async_remote_copy(
                    src_ref=row_out.at[index],
                    dst_ref=arrived.at[n],
                    send_sem=send_sem.at[n],
                    recv_sem=recv_sem.at[n],
                    device_id=device(offset),
                    device_id_type=MESH,
                )
            )
            copies[-1].start()
        total = own
        for n, copy in enumerate(copies):
            copy.wait_recv()
            total = total + arrived[n]
        return total, copies

    own = jnp.sum(packed, axis=0, keepdims=True)
    pl.semaphore_wait(ready, len(further))
    own, sent_a = reduce_over(first, own, 0, first_in, first_send, first_recv)
    own, sent_b = reduce_over(second, own, 1, second_in, second_send, second_recv)

    spread = jnp.broadcast_to(own, (8, SITES))
    g = [
        jnp.broadcast_to(
            jnp.sum(
                jnp.where((lane == 2 * n + row) & (row < 2), spread, 0.0), axis=1, keepdims=True
            ),
            (8, SITES),
        )
        for n in range(9)
    ]
    g00, g01r, g01i, g11, g02r, g02i, g12r, g12i, g22 = g
    ib = 1.0 / (g00 + epsilon)
    kr = (g01r - mass_shift * epsilon) * ib
    ki = g01i * ib
    hr = kr + mass_shift
    hi = ki
    kk = kr * kr + ki * ki
    wp = (g11 - 2.0 * (kr * g01r + ki * g01i) + kk * g00) * ib
    n1 = wp + epsilon
    in1 = 1.0 / n1
    er = epsilon * hr * ib
    ei = epsilon * hi * ib
    tr = (g02r - (kr * g01r - ki * g01i)) * ib
    ti = (g02i - (kr * g01i + ki * g01r)) * ib
    sr = mass_shift * er + tr
    si = mass_shift * ei + ti
    both = ib * in1
    ur = (g12r - kr * g11 - (kr * g02r + ki * g02i) + kk * g01r) * both
    ui = (g12i - ki * g11 - (kr * g02i - ki * g02r) + kk * g01i) * both
    pr = ur - mass_shift * epsilon * in1
    pi = ui
    h11r = pr + mass_shift
    h11i = pi
    q2 = (g22 - 2.0 * (kr * g12r + ki * g12i) + kk * g11) * both
    cross = sr * (pr * er - pi * ei) + si * (pr * ei + pi * er)
    n2 = (
        q2
        + (sr * sr + si * si) * in1 * (g00 * ib)
        + (pr * pr + pi * pi) * (wp * in1)
        - 2.0 * (sr * tr + si * ti) * in1
        - 2.0 * (pr * ur + pi * ui)
        + 2.0 * cross * in1
        + epsilon
    )
    mr = hr * h11r - hi * h11i - sr
    mi = hr * h11i + hi * h11r - si
    idet = 1.0 / (mr * mr + mi * mi + n2 * (hr * hr + hi * hi + n1))
    x1r = -mr * idet
    x1i = mi * idet
    fr = h11r + kr
    fi = h11i + ki
    x0r = (fr * mr + fi * mi + hr * n2) * idet
    x0i = (fi * mr - fr * mi - hi * n2) * idet

    sol, res = [], []
    for r in range(RHS):
        c0r, c0i, c1r, c1i = (v[r : r + 1, :] for v in (x0r, x0i, x1r, x1i))
        d0r = 1.0 - mass_shift * c0r
        d0i = -mass_shift * c0i
        d1r = mass_shift * c1r + c0r
        d1i = mass_shift * c1i + c0i
        ar, ai = parts(0, r)
        br, bi = parts(1, r)
        cr, ci = parts(2, r)
        sol.append(c0r * ar - c0i * ai + c1r * br - c1i * bi)
        sol.append(c0r * ai + c0i * ar + c1r * bi + c1i * br)
        res.append(d0r * ar - d0i * ai - (d1r * br - d1i * bi) - (c1r * cr - c1i * ci))
        res.append(d0r * ai + d0i * ar - (d1r * bi + d1i * br) - (c1r * ci + c1i * cr))
    both_ref[0] = jnp.concatenate(sol).T
    both_ref[1] = jnp.concatenate(res).T
    for copy in halos + later + sent_a + sent_b:
        copy.wait_send()


def finish(both_ref, sol_ref, res_ref):
    sol_ref[...] = both_ref[0]
    res_ref[...] = both_ref[1]


def shards(sizes, right_side, link_blocks):
    first, second, _, _ = offsets_of(sizes)
    f32 = jnp.float32
    both = pl.pallas_call(
        functools.partial(kernel, sizes),
        out_shape=jax.ShapeDtypeStruct((2, SITES, VEC), f32),
        in_specs=[pl.BlockSpec(memory_space=pl.ANY)] * 2,
        out_specs=pl.BlockSpec(memory_space=pltpu.VMEM),
        scratch_shapes=[
            pltpu.VMEM((9, 2, DOF, DOF, SITES), f32),
            pltpu.VMEM((SITES, VEC), f32),
            pltpu.VMEM((3, VEC, SITES), f32),
            pltpu.VMEM((9, RHS, 3, DOF, SITES), f32),
            pltpu.VMEM((DOF, 6, 8, SITES), f32),
            pltpu.VMEM((2, 2, VEC, SITES), f32),
            pltpu.VMEM((2, 2, 64, SITES), f32),
            pltpu.VMEM((2, 2, 64, SITES), f32),
            pltpu.VMEM((2, 2, 16, SITES), f32),
            pltpu.VMEM((2, 2, 16, SITES), f32),
            pltpu.VMEM((2, 1, SITES), f32),
            pltpu.VMEM((len(first), 1, SITES), f32),
            pltpu.VMEM((len(second), 1, SITES), f32),
            pltpu.SemaphoreType.DMA((9,)),
            pltpu.SemaphoreType.DMA,
            pltpu.SemaphoreType.DMA((2, 6)),
            pltpu.SemaphoreType.DMA((2, 6)),
            pltpu.SemaphoreType.DMA((len(first),)),
            pltpu.SemaphoreType.DMA((len(first),)),
            pltpu.SemaphoreType.DMA((len(second),)),
            pltpu.SemaphoreType.DMA((len(second),)),
            pltpu.SemaphoreType.REGULAR,
        ],
        compiler_params=pltpu.CompilerParams(
            collective_id=0, has_side_effects=True, vmem_limit_bytes=54000 * 1024
        ),
    )(
        pltpu.with_memory_space_constraint(right_side.reshape(SITES, VEC), pltpu.HBM),
        pltpu.with_memory_space_constraint(link_blocks.reshape(9, 2, DOF, DOF, SITES), pltpu.HBM),
    )
    sol, res = pl.pallas_call(
        finish,
        out_shape=(jax.ShapeDtypeStruct((SITES, VEC), f32),) * 2,
        in_specs=[pl.BlockSpec(memory_space=pltpu.VMEM)],
        out_specs=(pl.BlockSpec(memory_space=pltpu.VMEM),) * 2,
        compiler_params=pltpu.CompilerParams(vmem_limit_bytes=4 * 1024 * 1024),
    )(both)
    return sol.reshape(right_side.shape), res.reshape(right_side.shape)


def solution(mesh):
    sizes = tuple(mesh.shape[name] for name in AXES)
    spec = P("xy", "gz", "ta", None, None)
    return jax.shard_map(
        functools.partial(shards, sizes),
        mesh=mesh,
        in_specs=(spec, P("xy", "gz", "ta", None, None, None, None, None)),
        out_specs=(spec, spec),
        check_vma=False,
    )
```

```python
import functools

import jax
import jax.numpy as jnp
from jax import lax
from jax.experimental import pallas as pl
from jax.experimental.pallas import tpu as pltpu
from jax.sharding import PartitionSpec as P

DOF = 32
RHS = 2
SITES = 128
VEC = 128
AXES = ("xy", "gz", "ta")
MESH = pl.DeviceIdType.MESH

mass_shift = 4.0
epsilon = 1e-06

LOADS = ((7, 9), (5, 7), (0, 1), (3, 5), (1, 3))
ZOWN, ZFAR, TFAR = 9, 10, 11
OWN_A = (0, 3, 4)
OWN_B = (ZOWN, 7, 8)
FAR = (1, 2, ZFAR, TFAR)


def offsets_of(sizes):
    nx, nz, nt = sizes
    first = [(d, 0, 0) for d in range(1, nx)]
    second = [(0, a, b) for a in range(nz) for b in range(nt) if (a, b) != (0, 0)]

    def hops(offset):
        return sum(min(d, n - d) for d, n in zip(offset, sizes))

    beside = [offset for offset in first + second if hops(offset) == 1]
    further = [offset for offset in first + second if hops(offset) == 2]

    def distance(offset):
        return (min(offset[0], nx - offset[0]) + 1) // 2 + hops((0,) + offset[1:])

    others = [(d, a, b) for d in range(nx) for a in range(nz) for b in range(nt)][1:]
    return first, second, beside, further, sorted(others, key=distance, reverse=True)


def turn(value, shift):
    return pltpu.roll(value, shift % SITES, 1)


def rows_of_sums(tiles, row):
    for half in (4, 2, 1):
        low = (row & half) == 0
        tiles = [
            jnp.where(low, tiles[i], pltpu.roll(tiles[i + half], half, 0))
            + jnp.where(low, pltpu.roll(tiles[i], 8 - half, 0), tiles[i + half])
            for i in range(half)
        ]
    return tiles[0]


def kernel(
    sizes,
    rhs_hbm,
    links_hbm,
    both_ref,
    links,
    start,
    field,
    near,
    partial,
    merged,
    totals,
    folds,
    z_out,
    t_out,
    halo_in,
    row_out,
    arrived,
    link_sem,
    start_sem,
    halo_send,
    halo_recv,
    sum_send,
    sum_recv,
    near_by,
    ready,
    known,
):
    here = [lax.axis_index(name) for name in AXES]
    first, second, beside, further, others = offsets_of(sizes)

    def device(offset):
        return tuple(
            here[i] if offset[i] == 0 else lax.rem(here[i] + (offset[i] % sizes[i]), sizes[i])
            for i in range(3)
        )

    def tell(offsets, semaphore):
        for offset in offsets:
            pl.semaphore_signal(
                semaphore, inc=1, device_id=device(offset), device_id_type=MESH
            )

    load = pltpu.make_async_copy(rhs_hbm, start, start_sem)
    load.start()
    barrier = pltpu.get_barrier_semaphore()
    tell(beside, barrier)
    for n, (begin, end) in enumerate(LOADS):
        for k in range(begin, end):
            pltpu.make_async_copy(links_hbm.at[k], links.at[k], link_sem.at[n]).start()

    def loaded(n):
        whole = links.at[pl.ds(LOADS[n][0], LOADS[n][1] - LOADS[n][0])]
        pltpu.make_async_copy(whole, whole, link_sem.at[n]).wait()

    lane = lax.broadcasted_iota(jnp.int32, (8, SITES), 1)
    row = lax.broadcasted_iota(jnp.int32, (8, SITES), 0)
    lane_z = (lane // 8) % 2
    lane_t = lane % 8

    def wide(mask, rows):
        return jnp.tile(mask, (rows // 8, 1)) if rows > 8 else mask

    def put(k, r, value):
        real = value[:32]
        imag = value[32:]
        near[k, r, 0] = real
        near[k, r, 1] = real + imag
        near[k, r, 2] = imag - real

    def landing(j, r, n):
        return pl.ds(*((0, 64), (64, 64), (128, 32), (160, 32), (192, 8), (200, 8))[n])

    def remote(j, r, n, src, offset):
        return pltpu.make_async_remote_copy(
            src_ref=src,
            dst_ref=halo_in.at[j, r, landing(j, r, n)],
            send_sem=halo_send,
            recv_sem=halo_recv.at[2 * j + r],
            device_id=device(offset),
            device_id_type=MESH,
        )

    def arrive(j, r):
        whole = halo_in.at[j, r]
        pltpu.make_async_copy(whole, whole, halo_recv.at[2 * j + r]).wait()

    z_is = [wide(lane_z == p, 32) for p in range(2)]
    t_is = [lane_t == p for p in range(8)]

    def pack(j, r, value):
        real, imag = value[:32], value[32:]
        z_out[j, r, 0] = jnp.where(z_is[0], real, turn(imag, 8))
        z_out[j, r, 1] = jnp.where(z_is[1], real, turn(imag, -8))
        ahead = value[:8]
        behind = value[56:]
        for g in range(1, 8):
            ahead = jnp.where(t_is[g], turn(value[8 * g : 8 * g + 8], g), ahead)
        for g in range(7):
            behind = jnp.where(t_is[g], turn(value[8 * g : 8 * g + 8], g - 7), behind)
        t_out[j, r, 0] = ahead
        t_out[j, r, 1] = behind

    def send_x(j, r):
        mine = field.at[j, pl.ds(64 * r, 64)]
        remote(j, r, 0, mine, (-1, 0, 0)).start()
        remote(j, r, 1, mine, (1, 0, 0)).start()

    def send_zt(j, r):
        remote(j, r, 2, z_out.at[j, r, 0], (0, -1, 0)).start()
        remote(j, r, 3, z_out.at[j, r, 1], (0, 1, 0)).start()
        remote(j, r, 4, t_out.at[j, r, 0], (0, 0, -1)).start()
        remote(j, r, 5, t_out.at[j, r, 1], (0, 0, 1)).start()

    def put_own(j, r):
        value = field[j, 64 * r : 64 * r + 64, :]
        real, imag = value[:32], value[32:]
        put(0, r, value)
        put(3, r, turn(value, -16))
        put(4, r, turn(value, 16))
        put(
            ZOWN,
            r,
            jnp.concatenate([jnp.where(z_is[0], turn(v, -8), turn(v, 8)) for v in (real, imag)]),
        )
        last, initial = wide(t_is[7], 64), wide(t_is[0], 64)
        put(7, r, jnp.where(last, 0.0, turn(value, -1)))
        put(8, r, jnp.where(initial, 0.0, turn(value, 1)))

    def put_far(j, r):
        put(1, r, halo_in[j, r, 0:64, :])
        put(2, r, halo_in[j, r, 64:128, :])
        ahead, behind = halo_in[j, r, 128:160, :], halo_in[j, r, 160:192, :]
        put(
            ZFAR,
            r,
            jnp.concatenate(
                (
                    jnp.where(z_is[1], turn(ahead, 8), turn(behind, -8)),
                    jnp.where(z_is[1], ahead, behind),
                )
            ),
        )
        ahead, behind = halo_in[j, r, 192:200, :], halo_in[j, r, 200:208, :]
        put(
            TFAR,
            r,
            jnp.concatenate(
                [
                    jnp.where(
                        t_is[7],
                        turn(ahead, 7 - g),
                        jnp.where(t_is[0], turn(behind, -g), 0.0),
                    )
                    for g in range(8)
                ]
            ),
        )

    def coupling(k, part, c, rows):
        return links[k, part, c, rows, :] if k < 9 else merged[k - 9, part, c, rows, :]

    def added(sums, value, real, imag, total):
        factors = (total, imag, real)
        for q in range(len(value)):
            term = factors[q % 3] * value[q]
            sums[q] = term if sums[q] is None else sums[q] + term

    def nearby(k, sides, rows):
        return [near[k, r, q, rows, :] for r in sides for q in range(3)]

    def sweep_own(terms, fresh):
        def body(block, carry):
            for half in range(2):
                sites = [block * 8 + half * 4 + i for i in range(4)]
                sums = [[None if fresh else partial[c, q] for q in range(6)] for c in sites]
                for k in terms:
                    for t in range(4):
                        rows = slice(8 * t, 8 * t + 8)
                        value = nearby(k, range(RHS), rows)
                        for i, c in enumerate(sites):
                            real, imag = coupling(k, 0, c, rows), coupling(k, 1, c, rows)
                            added(sums[i], value, real, imag, real + imag)
                for i, c in enumerate(sites):
                    for q in range(6):
                        partial[c, q] = sums[i][q]
            return carry

        lax.fori_loop(0, 4, body, 0)

    even, last_t = z_is[0][:8], t_is[7]

    def sweep_merging(along_t):
        def body(block, carry):
            for half in range(2):
                sites = [block * 8 + half * 4 + i for i in range(4)]
                if along_t:
                    sums = [[None] * 6 for c in sites]
                else:
                    sums = [[partial[c, q] for q in range(6)] for c in sites]
                for t in range(4):
                    rows = slice(8 * t, 8 * t + 8)
                    terms = (7, 8) if along_t else (ZOWN,)
                    values = [nearby(k, range(RHS), rows) for k in terms]
                    for i, c in enumerate(sites):
                        up, down = (
                            [links[k, part, c, rows, :] for part in range(2)]
                            for k in ((7, 8) if along_t else (5, 6))
                        )
                        if along_t:
                            pairs = (up, down)
                            slot, place = TFAR - 9, 3
                            far = [jnp.where(last_t, a, b) for a, b in zip(up, down)]
                        else:
                            pairs = ([jnp.where(even, a, b) for a, b in zip(up, down)],)
                            slot, place = ZFAR - 9, 2
                            far = [jnp.where(even, b, a) for a, b in zip(up, down)]
                            for part in range(2):
                                merged[ZOWN - 9, part, c, rows, :] = pairs[0][part]
                        for part in range(2):
                            merged[slot, part, c, rows, :] = far[part]
                        totals[place, c, rows, :] = far[0] + far[1]
                        for value, (real, imag) in zip(values, pairs):
                            added(sums[i], value, real, imag, real + imag)
                for i, c in enumerate(sites):
                    for q in range(6):
                        partial[c, q] = sums[i][q]
            return carry

        lax.fori_loop(0, 4, body, 0)

    def total_x():
        def body(block, carry):
            for i in range(4):
                c = block * 4 + i
                for n in range(2):
                    totals[n, c] = links[1 + n, 0, c] + links[1 + n, 1, c]
            return carry

        lax.fori_loop(0, 8, body, 0)

    def sweep_far(j, r):
        def body(block, carry):
            sites = [block * 8 + i for i in range(8)]
            sums = [[partial[c, 3 * r + q] for q in range(3)] for c in sites]
            for n, k in enumerate(FAR):
                for t in range(4):
                    rows = slice(8 * t, 8 * t + 8)
                    value = nearby(k, (r,), rows)
                    for i, c in enumerate(sites):
                        added(
                            sums[i],
                            value,
                            coupling(k, 0, c, rows),
                            coupling(k, 1, c, rows),
                            totals[n, c, rows, :],
                        )
            for i, c in enumerate(sites):
                folds[c, 0] = sums[i][0] - sums[i][1]
                folds[c, 1] = sums[i][0] + sums[i][2]
            return carry

        lax.fori_loop(0, 4, body, 0)
        for part in range(2):
            for block in range(4):
                place = 64 * r + 32 * part + 8 * block
                field[j + 1, place : place + 8, :] = rows_of_sums(
                    [folds[8 * block + i, part] for i in range(8)], row
                )

    def parts(j, r):
        return field[j, 64 * r : 64 * r + 32, :], field[j, 64 * r + 32 : 64 * r + 64, :]

    def folded(value):
        value = value[:8] + value[8:16] + value[16:24] + value[24:]
        return jnp.sum(value, axis=1, keepdims=True)

    def gram(pairs, r, packed):
        for n, i, j, kind in pairs:
            ar, ai = parts(i, r)
            br, bi = (ar, ai) if i == j else parts(j, r)
            value = ar * br + ai * bi if kind == 0 else ar * bi - ai * br
            packed = jnp.where(lane == 2 * n + r, folded(value), packed)
        return packed

    load.wait()
    begin = start[...].T
    field[0] = begin
    for r in range(RHS):
        pack(0, r, begin[64 * r : 64 * r + 64])
    pl.semaphore_wait(barrier, len(beside))
    for r in range(RHS):
        send_x(0, r)
        send_zt(0, r)
    tell(beside, near_by)
    for r in range(RHS):
        put_own(0, r)
    loaded(0)
    sweep_merging(True)
    loaded(1)
    sweep_merging(False)
    loaded(2)
    loaded(3)
    sweep_own(OWN_A, False)
    pl.semaphore_wait(near_by, len(beside))
    tell(further, ready)
    loaded(4)
    total_x()
    for r in range(RHS):
        arrive(0, r)
        put_far(0, r)
        sweep_far(0, r)
        send_x(1, r)
        pack(1, r, field[1, 64 * r : 64 * r + 64, :])
        send_zt(1, r)
    pl.semaphore_wait(ready, len(further))
    tell(second, known)
    for r in range(RHS):
        put_own(1, r)
    sweep_own(OWN_A, True)
    sweep_own(OWN_B, False)
    packed = jnp.zeros((8, SITES), jnp.float32)
    for r in range(RHS):
        packed = gram(((0, 0, 0, 0), (1, 0, 1, 0), (2, 0, 1, 1), (3, 1, 1, 0)), r, packed)
    for r in range(RHS):
        arrive(1, r)
        put_far(1, r)
        sweep_far(1, r)
        packed = gram(
            ((4, 0, 2, 0), (5, 0, 2, 1), (6, 1, 2, 0), (7, 1, 2, 1), (8, 2, 2, 0)), r, packed
        )

    row_out[...] = jnp.sum(packed, axis=0, keepdims=True)
    pl.semaphore_wait(known, len(second))
    for n, offset in enumerate(others):
        pltpu.make_async_remote_copy(
            src_ref=row_out,
            dst_ref=arrived.at[pl.ds(n, 1)],
            send_sem=sum_send,
            recv_sem=sum_recv,
            device_id=device(offset),
            device_id_type=MESH,
        ).start()
    own = row_out[...]
    whole = arrived.at[pl.ds(0, len(others))]
    pltpu.make_async_copy(whole, whole, sum_recv).wait()
    own = own + jnp.sum(arrived[0 : len(others), :], axis=0, keepdims=True)

    spread = jnp.broadcast_to(own, (8, SITES))
    g = [
        jnp.broadcast_to(
            jnp.sum(
                jnp.where((lane == 2 * n + row) & (row < 2), spread, 0.0), axis=1, keepdims=True
            ),
            (8, SITES),
        )
        for n in range(9)
    ]
    g00, g01r, g01i, g11, g02r, g02i, g12r, g12i, g22 = g
    ib = 1.0 / (g00 + epsilon)
    kr = (g01r - mass_shift * epsilon) * ib
    ki = g01i * ib
    hr = kr + mass_shift
    hi = ki
    kk = kr * kr + ki * ki
    wp = (g11 - 2.0 * (kr * g01r + ki * g01i) + kk * g00) * ib
    n1 = wp + epsilon
    in1 = 1.0 / n1
    er = epsilon * hr * ib
    ei = epsilon * hi * ib
    tr = (g02r - (kr * g01r - ki * g01i)) * ib
    ti = (g02i - (kr * g01i + ki * g01r)) * ib
    sr = mass_shift * er + tr
    si = mass_shift * ei + ti
    both = ib * in1
    ur = (g12r - kr * g11 - (kr * g02r + ki * g02i) + kk * g01r) * both
    ui = (g12i - ki * g11 - (kr * g02i - ki * g02r) + kk * g01i) * both
    pr = ur - mass_shift * epsilon * in1
    pi = ui
    h11r = pr + mass_shift
    h11i = pi
    q2 = (g22 - 2.0 * (kr * g12r + ki * g12i) + kk * g11) * both
    cross = sr * (pr * er - pi * ei) + si * (pr * ei + pi * er)
    n2 = (
        q2
        + (sr * sr + si * si) * in1 * (g00 * ib)
        + (pr * pr + pi * pi) * (wp * in1)
        - 2.0 * (sr * tr + si * ti) * in1
        - 2.0 * (pr * ur + pi * ui)
        + 2.0 * cross * in1
        + epsilon
    )
    mr = hr * h11r - hi * h11i - sr
    mi = hr * h11i + hi * h11r - si
    idet = 1.0 / (mr * mr + mi * mi + n2 * (hr * hr + hi * hi + n1))
    x1r = -mr * idet
    x1i = mi * idet
    fr = h11r + kr
    fi = h11i + ki
    x0r = (fr * mr + fi * mi + hr * n2) * idet
    x0i = (fi * mr - fr * mi - hi * n2) * idet

    sol, res = [], []
    for r in range(RHS):
        c0r, c0i, c1r, c1i = (v[r : r + 1, :] for v in (x0r, x0i, x1r, x1i))
        d0r = 1.0 - mass_shift * c0r
        d0i = -mass_shift * c0i
        d1r = mass_shift * c1r + c0r
        d1i = mass_shift * c1i + c0i
        ar, ai = parts(0, r)
        br, bi = parts(1, r)
        cr, ci = parts(2, r)
        sol.append(c0r * ar - c0i * ai + c1r * br - c1i * bi)
        sol.append(c0r * ai + c0i * ar + c1r * bi + c1i * br)
        res.append(d0r * ar - d0i * ai - (d1r * br - d1i * bi) - (c1r * cr - c1i * ci))
        res.append(d0r * ai + d0i * ar - (d1r * bi + d1i * br) - (c1r * ci + c1i * cr))
    both_ref[0] = jnp.concatenate(sol).T
    both_ref[1] = jnp.concatenate(res).T
    pltpu.make_async_copy(halo_in, halo_in, halo_send).wait()
    pltpu.make_async_copy(whole, whole, sum_send).wait()


def finish(both_ref, sol_ref, res_ref):
    sol_ref[...] = both_ref[0]
    res_ref[...] = both_ref[1]


def shards(sizes, right_side, link_blocks):
    others = offsets_of(sizes)[-1]
    f32 = jnp.float32
    both = pl.pallas_call(
        functools.partial(kernel, sizes),
        out_shape=jax.ShapeDtypeStruct((2, SITES, VEC), f32),
        in_specs=[pl.BlockSpec(memory_space=pl.ANY)] * 2,
        out_specs=pl.BlockSpec(memory_space=pltpu.VMEM),
        scratch_shapes=[
            pltpu.VMEM((9, 2, DOF, DOF, SITES), f32),
            pltpu.VMEM((SITES, VEC), f32),
            pltpu.VMEM((3, VEC, SITES), f32),
            pltpu.VMEM((12, RHS, 3, DOF, SITES), f32),
            pltpu.VMEM((DOF, 6, 8, SITES), f32),
            pltpu.VMEM((3, 2, DOF, DOF, SITES), f32),
            pltpu.VMEM((4, DOF, DOF, SITES), f32),
            pltpu.VMEM((DOF, 2, 8, SITES), f32),
            pltpu.VMEM((2, RHS, 2, 32, SITES), f32),
            pltpu.VMEM((2, RHS, 2, 8, SITES), f32),
            pltpu.VMEM((2, RHS, 208, SITES), f32),
            pltpu.VMEM((1, SITES), f32),
            pltpu.VMEM((len(others), SITES), f32),
            pltpu.SemaphoreType.DMA((len(LOADS),)),
            pltpu.SemaphoreType.DMA,
            pltpu.SemaphoreType.DMA,
            pltpu.SemaphoreType.DMA((2 * RHS,)),
            pltpu.SemaphoreType.DMA,
            pltpu.SemaphoreType.DMA,
            pltpu.SemaphoreType.REGULAR,
            pltpu.SemaphoreType.REGULAR,
            pltpu.SemaphoreType.REGULAR,
        ],
        compiler_params=pltpu.CompilerParams(
            collective_id=0, has_side_effects=True, vmem_limit_bytes=54000 * 1024
        ),
    )(
        pltpu.with_memory_space_constraint(right_side.reshape(SITES, VEC), pltpu.HBM),
        pltpu.with_memory_space_constraint(link_blocks.reshape(9, 2, DOF, DOF, SITES), pltpu.HBM),
    )
    sol, res = pl.pallas_call(
        finish,
        out_shape=(jax.ShapeDtypeStruct((SITES, VEC), f32),) * 2,
        in_specs=[pl.BlockSpec(memory_space=pltpu.VMEM)],
        out_specs=(pl.BlockSpec(memory_space=pltpu.VMEM),) * 2,
        compiler_params=pltpu.CompilerParams(vmem_limit_bytes=4 * 1024 * 1024),
    )(both)
    return sol.reshape(right_side.shape), res.reshape(right_side.shape)


def solution(mesh):
    sizes = tuple(mesh.shape[name] for name in AXES)
    spec = P("xy", "gz", "ta", None, None)
    return jax.shard_map(
        functools.partial(shards, sizes),
        mesh=mesh,
        in_specs=(spec, P("xy", "gz", "ta", None, None, None, None, None)),
        out_specs=(spec, spec),
        check_vma=False,
    )
```

```python
import functools

import jax
import jax.numpy as jnp
from jax import lax
from jax.experimental import pallas as pl
from jax.experimental.pallas import tpu as pltpu
from jax.sharding import PartitionSpec as P

DOF = 32
RHS = 2
SITES = 128
VEC = 128
AXES = ("xy", "gz", "ta")
MESH = pl.DeviceIdType.MESH

mass_shift = 4.0
epsilon = 1e-06

LOADS = ((7, 9), (5, 7), (0, 1), (3, 5), (1, 3))
ZOWN, ZFAR, TFAR = 9, 10, 11
OWN_A = (0, 3, 4)
OWN_B = (ZOWN, 7, 8)
CHIP, OUTER = 1, 2
FAR = (OUTER, ZFAR, TFAR)
GROUPS = 2


def offsets_of(sizes):
    nx, nz, nt = sizes
    first = [(d, 0, 0) for d in range(1, nx)]
    second = [(0, a, b) for a in range(nz) for b in range(nt) if (a, b) != (0, 0)]

    def hops(offset):
        return sum(min(d, n - d) for d, n in zip(offset, sizes))

    beside = [offset for offset in first + second if hops(offset) == 1]
    further = [offset for offset in first + second if hops(offset) == 2]

    def distance(offset):
        return (min(offset[0], nx - offset[0]) + 1) // 2 + hops((0,) + offset[1:])

    others = [(d, a, b) for d in range(nx) for a in range(nz) for b in range(nt)][1:]
    return first, second, beside, further, sorted(others, key=distance, reverse=True)


def turn(value, shift):
    return pltpu.roll(value, shift % SITES, 1)


def rows_of_sums(tiles, row):
    for half in (4, 2, 1):
        low = (row & half) == 0
        tiles = [
            jnp.where(low, tiles[i], pltpu.roll(tiles[i + half], half, 0))
            + jnp.where(low, pltpu.roll(tiles[i], 8 - half, 0), tiles[i + half])
            for i in range(half)
        ]
    return tiles[0]


def kernel(
    sizes,
    rhs_hbm,
    links_hbm,
    both_ref,
    links,
    start,
    field,
    near,
    partial,
    merged,
    totals,
    folds,
    upright,
    z_out,
    t_out,
    halo_in,
    row_out,
    arrived,
    link_sem,
    start_sem,
    halo_send,
    halo_recv,
    chip_recv,
    sum_send,
    sum_recv,
    near_by,
    ready,
    known,
):
    here = [lax.axis_index(name) for name in AXES]
    first, second, beside, further, others = offsets_of(sizes)

    def device(offset):
        return tuple(
            here[i] if offset[i] == 0 else lax.rem(here[i] + (offset[i] % sizes[i]), sizes[i])
            for i in range(3)
        )

    def tell(offsets, semaphore):
        for offset in offsets:
            pl.semaphore_signal(
                semaphore, inc=1, device_id=device(offset), device_id_type=MESH
            )

    load = pltpu.make_async_copy(rhs_hbm, start, start_sem)
    load.start()
    odd = lax.rem(here[0], 2)
    partner = (here[0] + 1 - 2 * odd, here[1], here[2])
    outer = (lax.rem(here[0] + sizes[0] - 1 + 2 * odd, sizes[0]), here[1], here[2])
    coupling_of = {CHIP: 1 + odd, OUTER: 2 - odd}

    barrier = pltpu.get_barrier_semaphore()
    tell(beside, barrier)
    for n, (begin, end) in enumerate(LOADS):
        for k in range(begin, end):
            pltpu.make_async_copy(links_hbm.at[k], links.at[k], link_sem.at[n]).start()

    def loaded(n):
        whole = links.at[pl.ds(LOADS[n][0], LOADS[n][1] - LOADS[n][0])]
        pltpu.make_async_copy(whole, whole, link_sem.at[n]).wait()

    lane = lax.broadcasted_iota(jnp.int32, (8, SITES), 1)
    row = lax.broadcasted_iota(jnp.int32, (8, SITES), 0)
    lane_z = (lane // 8) % 2
    lane_t = lane % 8

    def wide(mask, rows):
        return jnp.tile(mask, (rows // 8, 1)) if rows > 8 else mask

    def put(k, r, value):
        real = value[:32]
        imag = value[32:]
        near[k, r, 0] = real
        near[k, r, 1] = real + imag
        near[k, r, 2] = imag - real

    def remote(j, r, place, rows, src, target, arrival):
        return pltpu.make_async_remote_copy(
            src_ref=src,
            dst_ref=halo_in.at[j, r, pl.ds(place, rows)],
            send_sem=halo_send,
            recv_sem=arrival.at[2 * j + r],
            device_id=target,
            device_id_type=MESH,
        )

    def arrive(j, r):
        rest = halo_in.at[j, r, pl.ds(64, 144)]
        pltpu.make_async_copy(rest, rest, halo_recv.at[2 * j + r]).wait()

    def arrive_chip(j, r):
        first_rows = halo_in.at[j, r, pl.ds(0, 64)]
        pltpu.make_async_copy(first_rows, first_rows, chip_recv.at[2 * j + r]).wait()
        put(CHIP, r, halo_in[j, r, 0:64, :])

    z_is = [wide(lane_z == p, 32) for p in range(2)]
    t_is = [lane_t == p for p in range(8)]

    def pack(j, r, value):
        real, imag = value[:32], value[32:]
        z_out[j, r, 0] = jnp.where(z_is[0], real, turn(imag, 8))
        z_out[j, r, 1] = jnp.where(z_is[1], real, turn(imag, -8))
        ahead = value[:8]
        behind = value[56:]
        for g in range(1, 8):
            ahead = jnp.where(t_is[g], turn(value[8 * g : 8 * g + 8], g), ahead)
        for g in range(7):
            behind = jnp.where(t_is[g], turn(value[8 * g : 8 * g + 8], g - 7), behind)
        t_out[j, r, 0] = ahead
        t_out[j, r, 1] = behind

    def send_x(j, r):
        mine = field.at[j, pl.ds(64 * r, 64)]
        remote(j, r, 64, 64, mine, outer, halo_recv).start()

    def send_chip(j, r):
        mine = field.at[j, pl.ds(64 * r, 64)]
        remote(j, r, 0, 64, mine, partner, chip_recv).start()

    def send_zt(j, r):
        for n in range(2):
            step = 2 * n - 1
            target = device((0, step, 0))
            remote(j, r, 128 + 32 * n, 32, z_out.at[j, r, n], target, halo_recv).start()
            target = device((0, 0, step))
            remote(j, r, 192 + 8 * n, 8, t_out.at[j, r, n], target, halo_recv).start()

    def put_own(j, r):
        value = field[j, 64 * r : 64 * r + 64, :]
        real, imag = value[:32], value[32:]
        put(0, r, value)
        put(3, r, turn(value, -16))
        put(4, r, turn(value, 16))
        put(
            ZOWN,
            r,
            jnp.concatenate([jnp.where(z_is[0], turn(v, -8), turn(v, 8)) for v in (real, imag)]),
        )
        last, initial = wide(t_is[7], 64), wide(t_is[0], 64)
        put(7, r, jnp.where(last, 0.0, turn(value, -1)))
        put(8, r, jnp.where(initial, 0.0, turn(value, 1)))

    def put_far(j, r):
        put(OUTER, r, halo_in[j, r, 64:128, :])
        ahead, behind = halo_in[j, r, 128:160, :], halo_in[j, r, 160:192, :]
        put(
            ZFAR,
            r,
            jnp.concatenate(
                (
                    jnp.where(z_is[1], turn(ahead, 8), turn(behind, -8)),
                    jnp.where(z_is[1], ahead, behind),
                )
            ),
        )
        ahead, behind = halo_in[j, r, 192:200, :], halo_in[j, r, 200:208, :]
        put(
            TFAR,
            r,
            jnp.concatenate(
                [
                    jnp.where(
                        t_is[7],
                        turn(ahead, 7 - g),
                        jnp.where(t_is[0], turn(behind, -g), 0.0),
                    )
                    for g in range(8)
                ]
            ),
        )

    def coupling(k, part, c, rows):
        if k >= 9:
            return merged[k - 9, part, c, rows, :]
        return links[coupling_of.get(k, k), part, c, rows, :]

    def added(sums, value, real, imag, total):
        factors = (total, imag, real)
        for q in range(len(value)):
            term = factors[q % 3] * value[q]
            sums[q] = term if sums[q] is None else sums[q] + term

    def nearby(k, sides, rows):
        return [near[k, r, q, rows, :] for r in sides for q in range(3)]

    def sweep_own(terms, fresh):
        def body(block, carry):
            for half in range(2):
                sites = [block * 8 + half * 4 + i for i in range(4)]
                sums = [[None if fresh else partial[c, q] for q in range(6)] for c in sites]
                for k in terms:
                    for t in range(4):
                        rows = slice(8 * t, 8 * t + 8)
                        value = nearby(k, range(RHS), rows)
                        for i, c in enumerate(sites):
                            real, imag = coupling(k, 0, c, rows), coupling(k, 1, c, rows)
                            added(sums[i], value, real, imag, real + imag)
                for i, c in enumerate(sites):
                    for q in range(6):
                        partial[c, q] = sums[i][q]
            return carry

        lax.fori_loop(0, 4, body, 0)

    even, last_t = z_is[0][:8], t_is[7]

    def sweep_merging(along_t):
        def body(block, carry):
            for half in range(2):
                sites = [block * 8 + half * 4 + i for i in range(4)]
                if along_t:
                    sums = [[None] * 6 for c in sites]
                else:
                    sums = [[partial[c, q] for q in range(6)] for c in sites]
                for t in range(4):
                    rows = slice(8 * t, 8 * t + 8)
                    terms = (7, 8) if along_t else (ZOWN,)
                    values = [nearby(k, range(RHS), rows) for k in terms]
                    for i, c in enumerate(sites):
                        up, down = (
                            [links[k, part, c, rows, :] for part in range(2)]
                            for k in ((7, 8) if along_t else (5, 6))
                        )
                        if along_t:
                            pairs = (up, down)
                            slot, place = TFAR - 9, 2
                            far = [jnp.where(last_t, a, b) for a, b in zip(up, down)]
                        else:
                            pairs = ([jnp.where(even, a, b) for a, b in zip(up, down)],)
                            slot, place = ZFAR - 9, 1
                            far = [jnp.where(even, b, a) for a, b in zip(up, down)]
                            for part in range(2):
                                merged[ZOWN - 9, part, c, rows, :] = pairs[0][part]
                        for part in range(2):
                            merged[slot, part, c, rows, :] = far[part]
                        totals[place, c, rows, :] = far[0] + far[1]
                        for value, (real, imag) in zip(values, pairs):
                            added(sums[i], value, real, imag, real + imag)
                for i, c in enumerate(sites):
                    for q in range(6):
                        partial[c, q] = sums[i][q]
            return carry

        lax.fori_loop(0, 4, body, 0)

    def total_outer():
        def body(block, carry):
            for i in range(4):
                c = block * 4 + i
                totals[0, c] = coupling(OUTER, 0, c, slice(None)) + coupling(
                    OUTER, 1, c, slice(None)
                )
            return carry

        lax.fori_loop(0, 8, body, 0)

    def sweep_far(j, r):
        def body(step, carry):
            for half in range(GROUPS):
                group(step * GROUPS + half)
            return carry

        def group(block):
            sites = [block * 8 + i for i in range(8)]
            sums = [[partial[c, 3 * r + q] for q in range(3)] for c in sites]
            for n, k in enumerate(FAR):
                for t in range(4):
                    rows = slice(8 * t, 8 * t + 8)
                    value = nearby(k, (r,), rows)
                    for i, c in enumerate(sites):
                        added(
                            sums[i],
                            value,
                            coupling(k, 0, c, rows),
                            coupling(k, 1, c, rows),
                            totals[n, c, rows, :],
                        )
            for i, c in enumerate(sites):
                folds[c, 0] = sums[i][0] - sums[i][1]
                folds[c, 1] = sums[i][0] + sums[i][2]

        lax.fori_loop(0, 4 // GROUPS, body, 0)
        for part in range(2):
            for block in range(4):
                place = 64 * r + 32 * part + 8 * block
                field[j + 1, place : place + 8, :] = rows_of_sums(
                    [folds[8 * block + i, part] for i in range(8)], row
                )

    def parts(j, r):
        return field[j, 64 * r : 64 * r + 32, :], field[j, 64 * r + 32 : 64 * r + 64, :]

    def folded(value):
        value = value[:8] + value[8:16] + value[16:24] + value[24:]
        return jnp.sum(value, axis=1, keepdims=True)

    def gram(pairs, r, packed):
        for n, i, j, kind in pairs:
            ar, ai = parts(i, r)
            br, bi = (ar, ai) if i == j else parts(j, r)
            value = ar * br + ai * bi if kind == 0 else ar * bi - ai * br
            packed = jnp.where(lane == 2 * n + r, folded(value), packed)
        return packed

    load.wait()
    begin = start[...].T
    field[0] = begin
    for r in range(RHS):
        pack(0, r, begin[64 * r : 64 * r + 64])
    pl.semaphore_wait(barrier, len(beside))
    for r in range(RHS):
        send_x(0, r)
        send_zt(0, r)
    for r in range(RHS):
        send_chip(0, r)
    tell(beside, near_by)
    for r in range(RHS):
        put_own(0, r)
    loaded(0)
    sweep_merging(True)
    loaded(1)
    sweep_merging(False)
    loaded(2)
    loaded(3)
    sweep_own(OWN_A, False)
    pl.semaphore_wait(near_by, len(beside))
    tell(further, ready)
    loaded(4)
    total_outer()
    for r in range(RHS):
        arrive_chip(0, r)
    sweep_own((CHIP,), False)
    for r in range(RHS):
        arrive(0, r)
        put_far(0, r)
        sweep_far(0, r)
        send_x(1, r)
        pack(1, r, field[1, 64 * r : 64 * r + 64, :])
        send_zt(1, r)
        send_chip(1, r)
    pl.semaphore_wait(ready, len(further))
    tell(second, known)
    for r in range(RHS):
        put_own(1, r)
    sweep_own(OWN_A, True)
    sweep_own(OWN_B, False)
    for r in range(RHS):
        arrive_chip(1, r)
    sweep_own((CHIP,), False)
    packed = jnp.zeros((8, SITES), jnp.float32)
    for r in range(RHS):
        packed = gram(((0, 0, 0, 0), (1, 0, 1, 0), (2, 0, 1, 1), (3, 1, 1, 0)), r, packed)
    for r in range(RHS):
        arrive(1, r)
        put_far(1, r)
        sweep_far(1, r)
    for r in range(RHS):
        packed = gram(
            ((4, 0, 2, 0), (5, 0, 2, 1), (6, 1, 2, 0), (7, 1, 2, 1), (8, 2, 2, 0)), r, packed
        )

    row_out[...] = jnp.sum(packed, axis=0, keepdims=True)
    pl.semaphore_wait(known, len(second))
    for n, offset in enumerate(others):
        pltpu.make_async_remote_copy(
            src_ref=row_out,
            dst_ref=arrived.at[pl.ds(n, 1)],
            send_sem=sum_send,
            recv_sem=sum_recv,
            device_id=device(offset),
            device_id_type=MESH,
        ).start()
    is_real = (lax.broadcasted_iota(jnp.int32, (SITES, VEC), 1) // 32) % 2 == 0

    def rotated(value):
        return jnp.where(is_real, -turn(value, -32), turn(value, 32))

    upright[0] = rotated(start[...])
    for j in (1, 2):
        value = field[j].T
        upright[2 * j - 1] = value
        upright[2 * j] = rotated(value)
    own = row_out[...]
    whole = arrived.at[pl.ds(0, len(others))]
    pltpu.make_async_copy(whole, whole, sum_recv).wait()
    own = own + jnp.sum(arrived[0 : len(others), :], axis=0, keepdims=True)

    spread = jnp.broadcast_to(own, (8, SITES))

    def total(n, r):
        chosen = jnp.where(lane == 2 * n + r, spread, 0.0)
        return jnp.broadcast_to(jnp.sum(chosen, axis=1, keepdims=True), (8, SITES))

    g = [jnp.where(lane < 64, total(n, 0), total(n, 1)) for n in range(9)]
    g00, g01r, g01i, g11, g02r, g02i, g12r, g12i, g22 = g
    ib = 1.0 / (g00 + epsilon)
    kr = (g01r - mass_shift * epsilon) * ib
    ki = g01i * ib
    hr = kr + mass_shift
    hi = ki
    kk = kr * kr + ki * ki
    wp = (g11 - 2.0 * (kr * g01r + ki * g01i) + kk * g00) * ib
    n1 = wp + epsilon
    in1 = 1.0 / n1
    er = epsilon * hr * ib
    ei = epsilon * hi * ib
    tr = (g02r - (kr * g01r - ki * g01i)) * ib
    ti = (g02i - (kr * g01i + ki * g01r)) * ib
    sr = mass_shift * er + tr
    si = mass_shift * ei + ti
    both = ib * in1
    ur = (g12r - kr * g11 - (kr * g02r + ki * g02i) + kk * g01r) * both
    ui = (g12i - ki * g11 - (kr * g02i - ki * g02r) + kk * g01i) * both
    pr = ur - mass_shift * epsilon * in1
    pi = ui
    h11r = pr + mass_shift
    h11i = pi
    q2 = (g22 - 2.0 * (kr * g12r + ki * g12i) + kk * g11) * both
    cross = sr * (pr * er - pi * ei) + si * (pr * ei + pi * er)
    n2 = (
        q2
        + (sr * sr + si * si) * in1 * (g00 * ib)
        + (pr * pr + pi * pi) * (wp * in1)
        - 2.0 * (sr * tr + si * ti) * in1
        - 2.0 * (pr * ur + pi * ui)
        + 2.0 * cross * in1
        + epsilon
    )
    mr = hr * h11r - hi * h11i - sr
    mi = hr * h11i + hi * h11r - si
    idet = 1.0 / (mr * mr + mi * mi + n2 * (hr * hr + hi * hi + n1))
    x1r = -mr * idet
    x1i = mi * idet
    fr = h11r + kr
    fi = h11i + ki
    x0r = (fr * mr + fi * mi + hr * n2) * idet
    x0i = (fi * mr - fr * mi - hi * n2) * idet

    d0r = 1.0 - mass_shift * x0r
    d0i = -mass_shift * x0i
    d1r = mass_shift * x1r + x0r
    d1i = mass_shift * x1i + x0i
    for n in range(SITES // 8):
        rows = slice(8 * n, 8 * n + 8)
        a, ia = start[rows, :], upright[0, rows, :]
        b, ib_, c, ic = (upright[k, rows, :] for k in range(1, 5))
        both_ref[0, rows, :] = x0r * a + x0i * ia + x1r * b + x1i * ib_
        both_ref[1, rows, :] = (
            d0r * a + d0i * ia - (d1r * b + d1i * ib_) - (x1r * c + x1i * ic)
        )
    pltpu.make_async_copy(halo_in, halo_in, halo_send).wait()
    pltpu.make_async_copy(whole, whole, sum_send).wait()


def finish(both_ref, sol_ref, res_ref, sems):
    copies = [
        pltpu.make_async_copy(both_ref.at[n], out, sems.at[n])
        for n, out in enumerate((sol_ref, res_ref))
    ]
    for copy in copies:
        copy.start()
    for copy in copies:
        copy.wait()


def shards(sizes, right_side, link_blocks):
    others = offsets_of(sizes)[-1]
    f32 = jnp.float32
    both = pl.pallas_call(
        functools.partial(kernel, sizes),
        out_shape=jax.ShapeDtypeStruct((2, SITES, VEC), f32),
        in_specs=[pl.BlockSpec(memory_space=pl.ANY)] * 2,
        out_specs=pl.BlockSpec(memory_space=pltpu.VMEM),
        scratch_shapes=[
            pltpu.VMEM((9, 2, DOF, DOF, SITES), f32),
            pltpu.VMEM((SITES, VEC), f32),
            pltpu.VMEM((3, VEC, SITES), f32),
            pltpu.VMEM((12, RHS, 3, DOF, SITES), f32),
            pltpu.VMEM((DOF, 6, 8, SITES), f32),
            pltpu.VMEM((3, 2, DOF, DOF, SITES), f32),
            pltpu.VMEM((3, DOF, DOF, SITES), f32),
            pltpu.VMEM((DOF, 2, 8, SITES), f32),
            pltpu.VMEM((5, SITES, VEC), f32),
            pltpu.VMEM((2, RHS, 2, 32, SITES), f32),
            pltpu.VMEM((2, RHS, 2, 8, SITES), f32),
            pltpu.VMEM((2, RHS, 208, SITES), f32),
            pltpu.VMEM((1, SITES), f32),
            pltpu.VMEM((len(others), SITES), f32),
            pltpu.SemaphoreType.DMA((len(LOADS),)),
            pltpu.SemaphoreType.DMA,
            pltpu.SemaphoreType.DMA,
            pltpu.SemaphoreType.DMA((2 * RHS,)),
            pltpu.SemaphoreType.DMA((2 * RHS,)),
            pltpu.SemaphoreType.DMA,
            pltpu.SemaphoreType.DMA,
            pltpu.SemaphoreType.REGULAR,
            pltpu.SemaphoreType.REGULAR,
            pltpu.SemaphoreType.REGULAR,
        ],
        compiler_params=pltpu.CompilerParams(
            collective_id=0, has_side_effects=True, vmem_limit_bytes=54000 * 1024
        ),
    )(
        pltpu.with_memory_space_constraint(right_side.reshape(SITES, VEC), pltpu.HBM),
        pltpu.with_memory_space_constraint(link_blocks.reshape(9, 2, DOF, DOF, SITES), pltpu.HBM),
    )
    sol, res = pl.pallas_call(
        finish,
        out_shape=(jax.ShapeDtypeStruct((SITES, VEC), f32),) * 2,
        in_specs=[pl.BlockSpec(memory_space=pltpu.VMEM)],
        out_specs=(pl.BlockSpec(memory_space=pl.ANY),) * 2,
        scratch_shapes=[pltpu.SemaphoreType.DMA((2,))],
        compiler_params=pltpu.CompilerParams(vmem_limit_bytes=4 * 1024 * 1024),
    )(both)
    return sol.reshape(right_side.shape), res.reshape(right_side.shape)


def solution(mesh):
    sizes = tuple(mesh.shape[name] for name in AXES)
    spec = P("xy", "gz", "ta", None, None)
    return jax.shard_map(
        functools.partial(shards, sizes),
        mesh=mesh,
        in_specs=(spec, P("xy", "gz", "ta", None, None, None, None, None)),
        out_specs=(spec, spec),
        check_vma=False,
    )
```

```python
import functools

import jax
import jax.numpy as jnp
from jax import lax
from jax.experimental import pallas as pl
from jax.experimental.pallas import tpu as pltpu
from jax.sharding import PartitionSpec as P

DOF = 32
RHS = 2
SITES = 128
VEC = 128
AXES = ("xy", "gz", "ta")
MESH = pl.DeviceIdType.MESH

mass_shift = 4.0
epsilon = 1e-06

LOADS = ((7, 9), (5, 7), (0, 1), (3, 5), (1, 3))
ZOWN, ZFAR, TFAR = 9, 10, 11
OWN_A = (0, 3, 4)
OWN_B = (ZOWN, 7, 8)
CHIP, OUTER = 1, 2
FAR = (OUTER, ZFAR, TFAR)


def offsets_of(sizes):
    nx, nz, nt = sizes
    first = [(d, 0, 0) for d in range(1, nx)]
    second = [(0, a, b) for a in range(nz) for b in range(nt) if (a, b) != (0, 0)]

    def hops(offset):
        return sum(min(d, n - d) for d, n in zip(offset, sizes))

    beside = [offset for offset in first + second if hops(offset) == 1]
    further = [offset for offset in first + second if hops(offset) == 2]

    def distance(offset):
        return (min(offset[0], nx - offset[0]) + 1) // 2 + hops((0,) + offset[1:])

    others = [(d, a, b) for d in range(nx) for a in range(nz) for b in range(nt)][1:]
    return first, second, beside, further, sorted(others, key=distance, reverse=True)


def turn(value, shift):
    return pltpu.roll(value, shift % SITES, 1)


def rows_of_sums(tiles, row):
    for half in (4, 2, 1):
        low = (row & half) == 0
        tiles = [
            jnp.where(low, tiles[i], pltpu.roll(tiles[i + half], half, 0))
            + jnp.where(low, pltpu.roll(tiles[i], 8 - half, 0), tiles[i + half])
            for i in range(half)
        ]
    return tiles[0]


def kernel(
    sizes,
    rhs_hbm,
    links_hbm,
    both_ref,
    links,
    start,
    field,
    near,
    partial,
    merged,
    totals,
    upright,
    z_out,
    t_out,
    halo_in,
    row_out,
    arrived,
    link_sem,
    start_sem,
    halo_send,
    halo_recv,
    chip_recv,
    outer_recv,
    sum_send,
    sum_recv,
    near_by,
    ready,
    known,
):
    here = [lax.axis_index(name) for name in AXES]
    first, second, beside, further, others = offsets_of(sizes)

    def device(offset):
        return tuple(
            here[i] if offset[i] == 0 else lax.rem(here[i] + (offset[i] % sizes[i]), sizes[i])
            for i in range(3)
        )

    def tell(offsets, semaphore):
        for offset in offsets:
            pl.semaphore_signal(
                semaphore, inc=1, device_id=device(offset), device_id_type=MESH
            )

    load = pltpu.make_async_copy(rhs_hbm, start, start_sem)
    load.start()
    odd = lax.rem(here[0], 2)
    partner = (here[0] + 1 - 2 * odd, here[1], here[2])
    outer = (lax.rem(here[0] + sizes[0] - 1 + 2 * odd, sizes[0]), here[1], here[2])
    coupling_of = {CHIP: 1 + odd, OUTER: 2 - odd}

    barrier = pltpu.get_barrier_semaphore()
    tell(beside, barrier)
    for n, (begin, end) in enumerate(LOADS):
        for k in range(begin, end):
            pltpu.make_async_copy(links_hbm.at[k], links.at[k], link_sem.at[n]).start()

    def loaded(n):
        whole = links.at[pl.ds(LOADS[n][0], LOADS[n][1] - LOADS[n][0])]
        pltpu.make_async_copy(whole, whole, link_sem.at[n]).wait()

    lane = lax.broadcasted_iota(jnp.int32, (8, SITES), 1)
    row = lax.broadcasted_iota(jnp.int32, (8, SITES), 0)
    lane_z = (lane // 8) % 2
    lane_t = lane % 8

    def wide(mask, rows):
        return jnp.tile(mask, (rows // 8, 1)) if rows > 8 else mask

    def put(k, r, value):
        real = value[:32]
        imag = value[32:]
        near[k, r, 0] = real
        near[k, r, 1] = real + imag
        near[k, r, 2] = imag - real

    def remote(j, r, place, rows, src, target, arrival):
        return pltpu.make_async_remote_copy(
            src_ref=src,
            dst_ref=halo_in.at[j, r, pl.ds(place, rows)],
            send_sem=halo_send,
            recv_sem=arrival.at[2 * j + r],
            device_id=target,
            device_id_type=MESH,
        )

    def arrive(j, r):
        rest = halo_in.at[j, r, pl.ds(128, 80)]
        pltpu.make_async_copy(rest, rest, halo_recv.at[2 * j + r]).wait()

    def arrive_outer(j, r):
        rest = halo_in.at[j, r, pl.ds(64, 64)]
        pltpu.make_async_copy(rest, rest, outer_recv.at[2 * j + r]).wait()
        put(OUTER, r, halo_in[j, r, 64:128, :])

    def arrive_chip(j, r):
        first_rows = halo_in.at[j, r, pl.ds(0, 64)]
        pltpu.make_async_copy(first_rows, first_rows, chip_recv.at[2 * j + r]).wait()
        put(CHIP, r, halo_in[j, r, 0:64, :])

    z_is = [wide(lane_z == p, 32) for p in range(2)]
    t_is = [lane_t == p for p in range(8)]

    def pack(j, r, value):
        real, imag = value[:32], value[32:]
        z_out[j, r, 0] = jnp.where(z_is[0], real, turn(imag, 8))
        z_out[j, r, 1] = jnp.where(z_is[1], real, turn(imag, -8))
        ahead = value[:8]
        behind = value[56:]
        for g in range(1, 8):
            ahead = jnp.where(t_is[g], turn(value[8 * g : 8 * g + 8], g), ahead)
        for g in range(7):
            behind = jnp.where(t_is[g], turn(value[8 * g : 8 * g + 8], g - 7), behind)
        t_out[j, r, 0] = ahead
        t_out[j, r, 1] = behind

    def send_x(j, r):
        mine = field.at[j, pl.ds(64 * r, 64)]
        remote(j, r, 64, 64, mine, outer, outer_recv).start()

    def send_chip(j, r):
        mine = field.at[j, pl.ds(64 * r, 64)]
        remote(j, r, 0, 64, mine, partner, chip_recv).start()

    def send_zt(j, r):
        for n in range(2):
            step = 2 * n - 1
            target = device((0, step, 0))
            remote(j, r, 128 + 32 * n, 32, z_out.at[j, r, n], target, halo_recv).start()
            target = device((0, 0, step))
            remote(j, r, 192 + 8 * n, 8, t_out.at[j, r, n], target, halo_recv).start()

    def put_own(j, r):
        value = field[j, 64 * r : 64 * r + 64, :]
        real, imag = value[:32], value[32:]
        put(0, r, value)
        put(3, r, turn(value, -16))
        put(4, r, turn(value, 16))
        put(
            ZOWN,
            r,
            jnp.concatenate([jnp.where(z_is[0], turn(v, -8), turn(v, 8)) for v in (real, imag)]),
        )
        last, initial = wide(t_is[7], 64), wide(t_is[0], 64)
        put(7, r, jnp.where(last, 0.0, turn(value, -1)))
        put(8, r, jnp.where(initial, 0.0, turn(value, 1)))

    def put_far(j, r):
        ahead, behind = halo_in[j, r, 128:160, :], halo_in[j, r, 160:192, :]
        put(
            ZFAR,
            r,
            jnp.concatenate(
                (
                    jnp.where(z_is[1], turn(ahead, 8), turn(behind, -8)),
                    jnp.where(z_is[1], ahead, behind),
                )
            ),
        )
        ahead, behind = halo_in[j, r, 192:200, :], halo_in[j, r, 200:208, :]
        put(
            TFAR,
            r,
            jnp.concatenate(
                [
                    jnp.where(
                        t_is[7],
                        turn(ahead, 7 - g),
                        jnp.where(t_is[0], turn(behind, -g), 0.0),
                    )
                    for g in range(8)
                ]
            ),
        )

    def coupling(k, part, c, rows):
        if k >= 9:
            return merged[k - 9, part, c, rows, :]
        return links[coupling_of.get(k, k), part, c, rows, :]

    def added(sums, value, real, imag, total):
        factors = (total, imag, real)
        for q in range(len(value)):
            term = factors[q % 3] * value[q]
            sums[q] = term if sums[q] is None else sums[q] + term

    def nearby(k, sides, rows):
        return [near[k, r, q, rows, :] for r in sides for q in range(3)]

    def sweep_own(terms, fresh):
        def body(block, carry):
            for half in range(2):
                sites = [block * 8 + half * 4 + i for i in range(4)]
                sums = [[None if fresh else partial[c, q] for q in range(6)] for c in sites]
                for k in terms:
                    for t in range(4):
                        rows = slice(8 * t, 8 * t + 8)
                        value = nearby(k, range(RHS), rows)
                        for i, c in enumerate(sites):
                            real, imag = coupling(k, 0, c, rows), coupling(k, 1, c, rows)
                            added(sums[i], value, real, imag, real + imag)
                for i, c in enumerate(sites):
                    for q in range(6):
                        partial[c, q] = sums[i][q]
            return carry

        lax.fori_loop(0, 4, body, 0)

    even, last_t = z_is[0][:8], t_is[7]

    def sweep_merging(along_t):
        def body(block, carry):
            for half in range(2):
                sites = [block * 8 + half * 4 + i for i in range(4)]
                if along_t:
                    sums = [[None] * 6 for c in sites]
                else:
                    sums = [[partial[c, q] for q in range(6)] for c in sites]
                for t in range(4):
                    rows = slice(8 * t, 8 * t + 8)
                    terms = (7, 8) if along_t else (ZOWN,)
                    values = [nearby(k, range(RHS), rows) for k in terms]
                    for i, c in enumerate(sites):
                        up, down = (
                            [links[k, part, c, rows, :] for part in range(2)]
                            for k in ((7, 8) if along_t else (5, 6))
                        )
                        if along_t:
                            pairs = (up, down)
                            slot, place = TFAR - 9, 2
                            far = [jnp.where(last_t, a, b) for a, b in zip(up, down)]
                        else:
                            pairs = ([jnp.where(even, a, b) for a, b in zip(up, down)],)
                            slot, place = ZFAR - 9, 1
                            far = [jnp.where(even, b, a) for a, b in zip(up, down)]
                            for part in range(2):
                                merged[ZOWN - 9, part, c, rows, :] = pairs[0][part]
                        for part in range(2):
                            merged[slot, part, c, rows, :] = far[part]
                        totals[place, c, rows, :] = far[0] + far[1]
                        for value, (real, imag) in zip(values, pairs):
                            added(sums[i], value, real, imag, real + imag)
                for i, c in enumerate(sites):
                    for q in range(6):
                        partial[c, q] = sums[i][q]
            return carry

        lax.fori_loop(0, 4, body, 0)

    def total_outer():
        def body(block, carry):
            for i in range(4):
                c = block * 4 + i
                totals[0, c] = coupling(OUTER, 0, c, slice(None)) + coupling(
                    OUTER, 1, c, slice(None)
                )
            return carry

        lax.fori_loop(0, 8, body, 0)

    def sweep_far(r, terms):
        def body(step, carry):
            for half in range(2):
                sites = [step * 16 + half * 8 + i for i in range(8)]
                sums = [[partial[c, 3 * r + q] for q in range(3)] for c in sites]
                for k in terms:
                    for t in range(4):
                        rows = slice(8 * t, 8 * t + 8)
                        value = nearby(k, (r,), rows)
                        for i, c in enumerate(sites):
                            added(
                                sums[i],
                                value,
                                coupling(k, 0, c, rows),
                                coupling(k, 1, c, rows),
                                totals[FAR.index(k), c, rows, :],
                            )
                for i, c in enumerate(sites):
                    for q in range(3):
                        partial[c, 3 * r + q] = sums[i][q]
            return carry

        lax.fori_loop(0, 2, body, 0)

    def finish_far(j, r):
        for block in range(4):
            sums = [[partial[8 * block + i, 3 * r + q] for q in range(3)] for i in range(8)]
            place = 64 * r + 8 * block
            field[j + 1, place : place + 8, :] = rows_of_sums([a - b for a, b, _ in sums], row)
            field[j + 1, place + 32 : place + 40, :] = rows_of_sums(
                [a + b for a, _, b in sums], row
            )

    def from_outer(j, r):
        arrive_outer(j, r)
        sweep_far(r, (OUTER,))

    def from_zt(j, r):
        arrive(j, r)
        put_far(j, r)
        sweep_far(r, (ZFAR, TFAR))

    def far_terms(j, r):
        @pl.when(odd == 0)
        def _():
            from_outer(j, r)
            from_zt(j, r)

        @pl.when(odd == 1)
        def _():
            from_zt(j, r)
            from_outer(j, r)

        finish_far(j, r)

    def parts(j, r):
        return field[j, 64 * r : 64 * r + 32, :], field[j, 64 * r + 32 : 64 * r + 64, :]

    def folded(value):
        value = value[:8] + value[8:16] + value[16:24] + value[24:]
        return jnp.sum(value, axis=1, keepdims=True)

    def gram(pairs, r, packed):
        for n, i, j, kind in pairs:
            ar, ai = parts(i, r)
            br, bi = (ar, ai) if i == j else parts(j, r)
            value = ar * br + ai * bi if kind == 0 else ar * bi - ai * br
            packed = jnp.where(lane == 2 * n + r, folded(value), packed)
        return packed

    load.wait()
    begin = start[...].T
    field[0] = begin
    for r in range(RHS):
        pack(0, r, begin[64 * r : 64 * r + 64])
    pl.semaphore_wait(barrier, len(beside))
    for r in range(RHS):
        send_x(0, r)
        send_zt(0, r)
    for r in range(RHS):
        send_chip(0, r)
    tell(beside, near_by)
    for r in range(RHS):
        put_own(0, r)
    loaded(0)
    sweep_merging(True)
    loaded(1)
    sweep_merging(False)
    loaded(2)
    loaded(3)
    sweep_own(OWN_A, False)
    pl.semaphore_wait(near_by, len(beside))
    tell(further, ready)
    loaded(4)
    total_outer()
    for r in range(RHS):
        arrive_chip(0, r)
    sweep_own((CHIP,), False)
    for r in range(RHS):
        far_terms(0, r)
        send_x(1, r)
        pack(1, r, field[1, 64 * r : 64 * r + 64, :])
        send_zt(1, r)
        send_chip(1, r)
    pl.semaphore_wait(ready, len(further))
    tell(second, known)
    for r in range(RHS):
        put_own(1, r)
    sweep_own(OWN_A, True)
    sweep_own(OWN_B, False)
    for r in range(RHS):
        arrive_chip(1, r)
    sweep_own((CHIP,), False)
    packed = jnp.zeros((8, SITES), jnp.float32)
    for r in range(RHS):
        packed = gram(((0, 0, 0, 0), (1, 0, 1, 0), (2, 0, 1, 1), (3, 1, 1, 0)), r, packed)
    for r in range(RHS):
        far_terms(1, r)
    for r in range(RHS):
        packed = gram(
            ((4, 0, 2, 0), (5, 0, 2, 1), (6, 1, 2, 0), (7, 1, 2, 1), (8, 2, 2, 0)), r, packed
        )

    row_out[...] = jnp.sum(packed, axis=0, keepdims=True)
    pl.semaphore_wait(known, len(second))
    for n, offset in enumerate(others):
        pltpu.make_async_remote_copy(
            src_ref=row_out,
            dst_ref=arrived.at[pl.ds(n, 1)],
            send_sem=sum_send,
            recv_sem=sum_recv,
            device_id=device(offset),
            device_id_type=MESH,
        ).start()
    is_real = (lax.broadcasted_iota(jnp.int32, (SITES, VEC), 1) // 32) % 2 == 0

    def rotated(value):
        return jnp.where(is_real, -turn(value, -32), turn(value, 32))

    upright[0] = rotated(start[...])
    for j in (1, 2):
        value = field[j].T
        upright[2 * j - 1] = value
        upright[2 * j] = rotated(value)
    own = row_out[...]
    whole = arrived.at[pl.ds(0, len(others))]
    pltpu.make_async_copy(whole, whole, sum_recv).wait()
    own = own + jnp.sum(arrived[0 : len(others), :], axis=0, keepdims=True)

    spread = jnp.broadcast_to(own, (8, SITES))

    def total(n, r):
        chosen = jnp.where(lane == 2 * n + r, spread, 0.0)
        return jnp.broadcast_to(jnp.sum(chosen, axis=1, keepdims=True), (8, SITES))

    g = [jnp.where(lane < 64, total(n, 0), total(n, 1)) for n in range(9)]
    g00, g01r, g01i, g11, g02r, g02i, g12r, g12i, g22 = g
    ib = 1.0 / (g00 + epsilon)
    kr = (g01r - mass_shift * epsilon) * ib
    ki = g01i * ib
    hr = kr + mass_shift
    hi = ki
    kk = kr * kr + ki * ki
    wp = (g11 - 2.0 * (kr * g01r + ki * g01i) + kk * g00) * ib
    n1 = wp + epsilon
    in1 = 1.0 / n1
    er = epsilon * hr * ib
    ei = epsilon * hi * ib
    tr = (g02r - (kr * g01r - ki * g01i)) * ib
    ti = (g02i - (kr * g01i + ki * g01r)) * ib
    sr = mass_shift * er + tr
    si = mass_shift * ei + ti
    both = ib * in1
    ur = (g12r - kr * g11 - (kr * g02r + ki * g02i) + kk * g01r) * both
    ui = (g12i - ki * g11 - (kr * g02i - ki * g02r) + kk * g01i) * both
    pr = ur - mass_shift * epsilon * in1
    pi = ui
    h11r = pr + mass_shift
    h11i = pi
    q2 = (g22 - 2.0 * (kr * g12r + ki * g12i) + kk * g11) * both
    cross = sr * (pr * er - pi * ei) + si * (pr * ei + pi * er)
    n2 = (
        q2
        + (sr * sr + si * si) * in1 * (g00 * ib)
        + (pr * pr + pi * pi) * (wp * in1)
        - 2.0 * (sr * tr + si * ti) * in1
        - 2.0 * (pr * ur + pi * ui)
        + 2.0 * cross * in1
        + epsilon
    )
    mr = hr * h11r - hi * h11i - sr
    mi = hr * h11i + hi * h11r - si
    idet = 1.0 / (mr * mr + mi * mi + n2 * (hr * hr + hi * hi + n1))
    x1r = -mr * idet
    x1i = mi * idet
    fr = h11r + kr
    fi = h11i + ki
    x0r = (fr * mr + fi * mi + hr * n2) * idet
    x0i = (fi * mr - fr * mi - hi * n2) * idet

    d0r = 1.0 - mass_shift * x0r
    d0i = -mass_shift * x0i
    d1r = mass_shift * x1r + x0r
    d1i = mass_shift * x1i + x0i
    for n in range(SITES // 8):
        rows = slice(8 * n, 8 * n + 8)
        a, ia = start[rows, :], upright[0, rows, :]
        b, ib_, c, ic = (upright[k, rows, :] for k in range(1, 5))
        both_ref[0, rows, :] = x0r * a + x0i * ia + x1r * b + x1i * ib_
        both_ref[1, rows, :] = (
            d0r * a + d0i * ia - (d1r * b + d1i * ib_) - (x1r * c + x1i * ic)
        )
    pltpu.make_async_copy(halo_in, halo_in, halo_send).wait()
    pltpu.make_async_copy(whole, whole, sum_send).wait()


def finish(both_ref, sol_ref, res_ref, sems):
    copies = [
        pltpu.make_async_copy(both_ref.at[n], out, sems.at[n])
        for n, out in enumerate((sol_ref, res_ref))
    ]
    for copy in copies:
        copy.start()
    for copy in copies:
        copy.wait()


def shards(sizes, right_side, link_blocks):
    others = offsets_of(sizes)[-1]
    f32 = jnp.float32
    both = pl.pallas_call(
        functools.partial(kernel, sizes),
        out_shape=jax.ShapeDtypeStruct((2, SITES, VEC), f32),
        in_specs=[pl.BlockSpec(memory_space=pl.ANY)] * 2,
        out_specs=pl.BlockSpec(memory_space=pltpu.VMEM),
        scratch_shapes=[
            pltpu.VMEM((9, 2, DOF, DOF, SITES), f32),
            pltpu.VMEM((SITES, VEC), f32),
            pltpu.VMEM((3, VEC, SITES), f32),
            pltpu.VMEM((12, RHS, 3, DOF, SITES), f32),
            pltpu.VMEM((DOF, 6, 8, SITES), f32),
            pltpu.VMEM((3, 2, DOF, DOF, SITES), f32),
            pltpu.VMEM((3, DOF, DOF, SITES), f32),
            pltpu.VMEM((5, SITES, VEC), f32),
            pltpu.VMEM((2, RHS, 2, 32, SITES), f32),
            pltpu.VMEM((2, RHS, 2, 8, SITES), f32),
            pltpu.VMEM((2, RHS, 208, SITES), f32),
            pltpu.VMEM((1, SITES), f32),
            pltpu.VMEM((len(others), SITES), f32),
            pltpu.SemaphoreType.DMA((len(LOADS),)),
            pltpu.SemaphoreType.DMA,
            pltpu.SemaphoreType.DMA,
            pltpu.SemaphoreType.DMA((2 * RHS,)),
            pltpu.SemaphoreType.DMA((2 * RHS,)),
            pltpu.SemaphoreType.DMA((2 * RHS,)),
            pltpu.SemaphoreType.DMA,
            pltpu.SemaphoreType.DMA,
            pltpu.SemaphoreType.REGULAR,
            pltpu.SemaphoreType.REGULAR,
            pltpu.SemaphoreType.REGULAR,
        ],
        compiler_params=pltpu.CompilerParams(
            collective_id=0, has_side_effects=True, vmem_limit_bytes=54000 * 1024
        ),
    )(
        pltpu.with_memory_space_constraint(right_side.reshape(SITES, VEC), pltpu.HBM),
        pltpu.with_memory_space_constraint(link_blocks.reshape(9, 2, DOF, DOF, SITES), pltpu.HBM),
    )
    sol, res = pl.pallas_call(
        finish,
        out_shape=(jax.ShapeDtypeStruct((SITES, VEC), f32),) * 2,
        in_specs=[pl.BlockSpec(memory_space=pltpu.VMEM)],
        out_specs=(pl.BlockSpec(memory_space=pl.ANY),) * 2,
        scratch_shapes=[pltpu.SemaphoreType.DMA((2,))],
        compiler_params=pltpu.CompilerParams(vmem_limit_bytes=4 * 1024 * 1024),
    )(both)
    return sol.reshape(right_side.shape), res.reshape(right_side.shape)


def solution(mesh):
    sizes = tuple(mesh.shape[name] for name in AXES)
    spec = P("xy", "gz", "ta", None, None)
    return jax.shard_map(
        functools.partial(shards, sizes),
        mesh=mesh,
        in_specs=(spec, P("xy", "gz", "ta", None, None, None, None, None)),
        out_specs=(spec, spec),
        check_vma=False,
    )
```

```python
import functools

import jax
import jax.numpy as jnp
from jax import lax
from jax.experimental import pallas as pl
from jax.experimental.pallas import tpu as pltpu
from jax.sharding import PartitionSpec as P

DOF = 32
RHS = 2
SITES = 128
VEC = 128
AXES = ("xy", "gz", "ta")
MESH = pl.DeviceIdType.MESH

mass_shift = 4.0
epsilon = 1e-06

LOADS = ((0, 1), (7, 9), (5, 7), (3, 5), (1, 3))
ZOWN, ZFAR, TFAR = 9, 10, 11
OWN_A = (0, 3, 4)
OWN_B = (ZOWN, 7, 8)
CHIP, OUTER = 1, 2
FAR = (OUTER, ZFAR, TFAR)


def offsets_of(sizes):
    nx, nz, nt = sizes
    first = [(d, 0, 0) for d in range(1, nx)]
    second = [(0, a, b) for a in range(nz) for b in range(nt) if (a, b) != (0, 0)]

    def hops(offset):
        return sum(min(d, n - d) for d, n in zip(offset, sizes))

    beside = [offset for offset in first + second if hops(offset) == 1]
    further = [offset for offset in first + second if hops(offset) == 2]

    def distance(offset):
        return (min(offset[0], nx - offset[0]) + 1) // 2 + hops((0,) + offset[1:])

    others = [(d, a, b) for d in range(nx) for a in range(nz) for b in range(nt)][1:]
    return first, second, beside, further, sorted(others, key=distance, reverse=True)


def turn(value, shift):
    return pltpu.roll(value, shift % SITES, 1)


def rows_of_sums(tiles, row):
    for half in (4, 2, 1):
        low = (row & half) == 0
        tiles = [
            jnp.where(low, tiles[i], pltpu.roll(tiles[i + half], half, 0))
            + jnp.where(low, pltpu.roll(tiles[i], 8 - half, 0), tiles[i + half])
            for i in range(half)
        ]
    return tiles[0]


def kernel(
    sizes,
    rhs_hbm,
    links_hbm,
    both_ref,
    links,
    start,
    field,
    near,
    partial,
    merged,
    totals,
    upright,
    z_out,
    t_out,
    halo_in,
    row_out,
    arrived,
    link_sem,
    start_sem,
    halo_send,
    halo_recv,
    chip_recv,
    outer_recv,
    sum_send,
    sum_recv,
    near_by,
    ready,
    known,
):
    here = [lax.axis_index(name) for name in AXES]
    first, second, beside, further, others = offsets_of(sizes)

    def device(offset):
        return tuple(
            here[i] if offset[i] == 0 else lax.rem(here[i] + (offset[i] % sizes[i]), sizes[i])
            for i in range(3)
        )

    def tell(offsets, semaphore):
        for offset in offsets:
            pl.semaphore_signal(
                semaphore, inc=1, device_id=device(offset), device_id_type=MESH
            )

    load = pltpu.make_async_copy(rhs_hbm, start, start_sem)
    load.start()
    odd = lax.rem(here[0], 2)
    partner = (here[0] + 1 - 2 * odd, here[1], here[2])
    outer = (lax.rem(here[0] + sizes[0] - 1 + 2 * odd, sizes[0]), here[1], here[2])
    coupling_of = {CHIP: 1 + odd, OUTER: 2 - odd}

    barrier = pltpu.get_barrier_semaphore()
    tell(beside, barrier)
    for n, (begin, end) in enumerate(LOADS):
        for k in range(begin, end):
            pltpu.make_async_copy(links_hbm.at[k], links.at[k], link_sem.at[n]).start()

    def loaded(n):
        whole = links.at[pl.ds(LOADS[n][0], LOADS[n][1] - LOADS[n][0])]
        pltpu.make_async_copy(whole, whole, link_sem.at[n]).wait()

    lane = lax.broadcasted_iota(jnp.int32, (8, SITES), 1)
    row = lax.broadcasted_iota(jnp.int32, (8, SITES), 0)
    lane_z = (lane // 8) % 2
    lane_t = lane % 8

    def wide(mask, rows):
        return jnp.tile(mask, (rows // 8, 1)) if rows > 8 else mask

    def put(k, r, value):
        real = value[:32]
        imag = value[32:]
        near[k, r, 0] = real
        near[k, r, 1] = real + imag
        near[k, r, 2] = imag - real

    def remote(j, r, place, rows, src, target, arrival):
        return pltpu.make_async_remote_copy(
            src_ref=src,
            dst_ref=halo_in.at[j, r, pl.ds(place, rows)],
            send_sem=halo_send,
            recv_sem=arrival.at[2 * j + r],
            device_id=target,
            device_id_type=MESH,
        )

    def arrive(j, r):
        rest = halo_in.at[j, r, pl.ds(128, 80)]
        pltpu.make_async_copy(rest, rest, halo_recv.at[2 * j + r]).wait()

    def arrive_outer(j, r):
        rest = halo_in.at[j, r, pl.ds(64, 64)]
        pltpu.make_async_copy(rest, rest, outer_recv.at[2 * j + r]).wait()
        put(OUTER, r, halo_in[j, r, 64:128, :])

    def arrive_chip(j, r):
        first_rows = halo_in.at[j, r, pl.ds(0, 64)]
        pltpu.make_async_copy(first_rows, first_rows, chip_recv.at[2 * j + r]).wait()
        put(CHIP, r, halo_in[j, r, 0:64, :])

    z_is = [wide(lane_z == p, 32) for p in range(2)]
    t_is = [lane_t == p for p in range(8)]

    def pack(j, r, value):
        real, imag = value[:32], value[32:]
        z_out[j, r, 0] = jnp.where(z_is[0], real, turn(imag, 8))
        z_out[j, r, 1] = jnp.where(z_is[1], real, turn(imag, -8))
        ahead = value[:8]
        behind = value[56:]
        for g in range(1, 8):
            ahead = jnp.where(t_is[g], turn(value[8 * g : 8 * g + 8], g), ahead)
        for g in range(7):
            behind = jnp.where(t_is[g], turn(value[8 * g : 8 * g + 8], g - 7), behind)
        t_out[j, r, 0] = ahead
        t_out[j, r, 1] = behind

    def send_x(j, r):
        mine = field.at[j, pl.ds(64 * r, 64)]
        remote(j, r, 64, 64, mine, outer, outer_recv).start()

    def send_chip(j, r):
        mine = field.at[j, pl.ds(64 * r, 64)]
        remote(j, r, 0, 64, mine, partner, chip_recv).start()

    def send_t(j, r):
        for n in range(2):
            target = device((0, 0, 2 * n - 1))
            remote(j, r, 192 + 8 * n, 8, t_out.at[j, r, n], target, halo_recv).start()

    def send_z(j, sides, core):
        @pl.when(odd == core)
        def _():
            for r in sides:
                for n in range(2):
                    target = device((0, 2 * n - 1, 0))
                    remote(
                        j, r, 128 + 32 * n, 32, z_out.at[j, r, n], target, halo_recv
                    ).start()

    def put_own(j, r):
        value = field[j, 64 * r : 64 * r + 64, :]
        real, imag = value[:32], value[32:]
        put(0, r, value)
        put(3, r, turn(value, -16))
        put(4, r, turn(value, 16))
        put(
            ZOWN,
            r,
            jnp.concatenate([jnp.where(z_is[0], turn(v, -8), turn(v, 8)) for v in (real, imag)]),
        )
        last, initial = wide(t_is[7], 64), wide(t_is[0], 64)
        put(7, r, jnp.where(last, 0.0, turn(value, -1)))
        put(8, r, jnp.where(initial, 0.0, turn(value, 1)))

    def put_far(j, r):
        ahead, behind = halo_in[j, r, 128:160, :], halo_in[j, r, 160:192, :]
        put(
            ZFAR,
            r,
            jnp.concatenate(
                (
                    jnp.where(z_is[1], turn(ahead, 8), turn(behind, -8)),
                    jnp.where(z_is[1], ahead, behind),
                )
            ),
        )
        ahead, behind = halo_in[j, r, 192:200, :], halo_in[j, r, 200:208, :]
        put(
            TFAR,
            r,
            jnp.concatenate(
                [
                    jnp.where(
                        t_is[7],
                        turn(ahead, 7 - g),
                        jnp.where(t_is[0], turn(behind, -g), 0.0),
                    )
                    for g in range(8)
                ]
            ),
        )

    def coupling(k, part, c, rows):
        if k >= 9:
            return merged[k - 9, part, c, rows, :]
        return links[coupling_of.get(k, k), part, c, rows, :]

    def added(sums, value, real, imag, total):
        factors = (total, imag, real)
        for q in range(len(value)):
            term = factors[q % 3] * value[q]
            sums[q] = term if sums[q] is None else sums[q] + term

    def nearby(k, sides, rows):
        return [near[k, r, q, rows, :] for r in sides for q in range(3)]

    def sweep_own(terms, fresh):
        def body(block, carry):
            for half in range(2):
                sites = [block * 8 + half * 4 + i for i in range(4)]
                sums = [[None if fresh else partial[c, q] for q in range(6)] for c in sites]
                for k in terms:
                    for t in range(4):
                        rows = slice(8 * t, 8 * t + 8)
                        value = nearby(k, range(RHS), rows)
                        for i, c in enumerate(sites):
                            real, imag = coupling(k, 0, c, rows), coupling(k, 1, c, rows)
                            added(sums[i], value, real, imag, real + imag)
                for i, c in enumerate(sites):
                    for q in range(6):
                        partial[c, q] = sums[i][q]
            return carry

        lax.fori_loop(0, 4, body, 0)

    even, last_t = z_is[0][:8], t_is[7]

    def sweep_merging(along_t):
        def body(block, carry):
            for half in range(2):
                sites = [block * 8 + half * 4 + i for i in range(4)]
                sums = [[partial[c, q] for q in range(6)] for c in sites]
                for t in range(4):
                    rows = slice(8 * t, 8 * t + 8)
                    terms = (7, 8) if along_t else (ZOWN,)
                    values = [nearby(k, range(RHS), rows) for k in terms]
                    for i, c in enumerate(sites):
                        up, down = (
                            [links[k, part, c, rows, :] for part in range(2)]
                            for k in ((7, 8) if along_t else (5, 6))
                        )
                        if along_t:
                            pairs = (up, down)
                            slot, place = TFAR - 9, 2
                            far = [jnp.where(last_t, a, b) for a, b in zip(up, down)]
                        else:
                            pairs = ([jnp.where(even, a, b) for a, b in zip(up, down)],)
                            slot, place = ZFAR - 9, 1
                            far = [jnp.where(even, b, a) for a, b in zip(up, down)]
                            for part in range(2):
                                merged[ZOWN - 9, part, c, rows, :] = pairs[0][part]
                        for part in range(2):
                            merged[slot, part, c, rows, :] = far[part]
                        totals[place, c, rows, :] = far[0] + far[1]
                        for value, (real, imag) in zip(values, pairs):
                            added(sums[i], value, real, imag, real + imag)
                for i, c in enumerate(sites):
                    for q in range(6):
                        partial[c, q] = sums[i][q]
            return carry

        lax.fori_loop(0, 4, body, 0)

    def total_outer():
        def body(block, carry):
            for i in range(4):
                c = block * 4 + i
                totals[0, c] = coupling(OUTER, 0, c, slice(None)) + coupling(
                    OUTER, 1, c, slice(None)
                )
            return carry

        lax.fori_loop(0, 8, body, 0)

    def sweep_far(r, terms):
        def body(step, carry):
            for half in range(2):
                sites = [step * 16 + half * 8 + i for i in range(8)]
                sums = [[partial[c, 3 * r + q] for q in range(3)] for c in sites]
                for k in terms:
                    for t in range(4):
                        rows = slice(8 * t, 8 * t + 8)
                        value = nearby(k, (r,), rows)
                        for i, c in enumerate(sites):
                            added(
                                sums[i],
                                value,
                                coupling(k, 0, c, rows),
                                coupling(k, 1, c, rows),
                                totals[FAR.index(k), c, rows, :],
                            )
                for i, c in enumerate(sites):
                    for q in range(3):
                        partial[c, 3 * r + q] = sums[i][q]
            return carry

        lax.fori_loop(0, 2, body, 0)

    def finish_far(j, r):
        for block in range(4):
            sums = [[partial[8 * block + i, 3 * r + q] for q in range(3)] for i in range(8)]
            place = 64 * r + 8 * block
            field[j + 1, place : place + 8, :] = rows_of_sums([a - b for a, b, _ in sums], row)
            field[j + 1, place + 32 : place + 40, :] = rows_of_sums(
                [a + b for a, _, b in sums], row
            )

    def from_outer(j, r):
        arrive_outer(j, r)
        sweep_far(r, (OUTER,))

    def from_zt(j, r):
        arrive(j, r)
        put_far(j, r)
        sweep_far(r, (ZFAR, TFAR))

    def far_terms(j, r):
        @pl.when(odd == 0)
        def _():
            from_outer(j, r)
            from_zt(j, r)

        @pl.when(odd == 1)
        def _():
            from_zt(j, r)
            from_outer(j, r)

        finish_far(j, r)

    def parts(j, r):
        return field[j, 64 * r : 64 * r + 32, :], field[j, 64 * r + 32 : 64 * r + 64, :]

    def folded(value):
        value = value[:8] + value[8:16] + value[16:24] + value[24:]
        return jnp.sum(value, axis=1, keepdims=True)

    def gram(pairs, r, packed):
        for n, i, j, kind in pairs:
            ar, ai = parts(i, r)
            br, bi = (ar, ai) if i == j else parts(j, r)
            value = ar * br + ai * bi if kind == 0 else ar * bi - ai * br
            packed = jnp.where(lane == 2 * n + r, folded(value), packed)
        return packed

    load.wait()
    begin = start[...].T
    field[0] = begin
    for r in range(RHS):
        pack(0, r, begin[64 * r : 64 * r + 64])
    pl.semaphore_wait(barrier, len(beside))
    for r in range(RHS):
        send_z(0, (r,), 0)
        send_x(0, r)
        send_t(0, r)
    for r in range(RHS):
        send_chip(0, r)
    tell(beside, near_by)
    for r in range(RHS):
        put_own(0, r)
    send_z(0, range(RHS), 1)
    loaded(0)
    sweep_own((0,), True)
    loaded(1)
    sweep_merging(True)
    loaded(2)
    sweep_merging(False)
    loaded(3)
    sweep_own((3, 4), False)
    pl.semaphore_wait(near_by, len(beside))
    tell(further, ready)
    loaded(4)
    total_outer()
    for r in range(RHS):
        arrive_chip(0, r)
    sweep_own((CHIP,), False)
    for r in range(RHS):
        far_terms(0, r)
        send_x(1, r)
        pack(1, r, field[1, 64 * r : 64 * r + 64, :])
        send_z(1, (r,), 0)
        send_t(1, r)
        send_chip(1, r)
    pl.semaphore_wait(ready, len(further))
    tell(second, known)
    for r in range(RHS):
        put_own(1, r)
    send_z(1, range(RHS), 1)
    sweep_own(OWN_A, True)
    sweep_own(OWN_B, False)
    for r in range(RHS):
        arrive_chip(1, r)
    sweep_own((CHIP,), False)
    packed = jnp.zeros((8, SITES), jnp.float32)
    for r in range(RHS):
        packed = gram(((0, 0, 0, 0), (1, 0, 1, 0), (2, 0, 1, 1), (3, 1, 1, 0)), r, packed)
    for r in range(RHS):
        far_terms(1, r)
    for r in range(RHS):
        packed = gram(
            ((4, 0, 2, 0), (5, 0, 2, 1), (6, 1, 2, 0), (7, 1, 2, 1), (8, 2, 2, 0)), r, packed
        )

    row_out[...] = jnp.sum(packed, axis=0, keepdims=True)
    pl.semaphore_wait(known, len(second))
    for n, offset in enumerate(others):
        pltpu.make_async_remote_copy(
            src_ref=row_out,
            dst_ref=arrived.at[pl.ds(n, 1)],
            send_sem=sum_send,
            recv_sem=sum_recv,
            device_id=device(offset),
            device_id_type=MESH,
        ).start()
    is_real = (lax.broadcasted_iota(jnp.int32, (SITES, VEC), 1) // 32) % 2 == 0

    def rotated(value):
        return jnp.where(is_real, -turn(value, -32), turn(value, 32))

    upright[0] = rotated(start[...])
    for j in (1, 2):
        value = field[j].T
        upright[2 * j - 1] = value
        upright[2 * j] = rotated(value)
    own = row_out[...]
    whole = arrived.at[pl.ds(0, len(others))]
    pltpu.make_async_copy(whole, whole, sum_recv).wait()
    own = own + jnp.sum(arrived[0 : len(others), :], axis=0, keepdims=True)

    spread = jnp.broadcast_to(own, (8, SITES))

    def total(n, r):
        chosen = jnp.where(lane == 2 * n + r, spread, 0.0)
        return jnp.broadcast_to(jnp.sum(chosen, axis=1, keepdims=True), (8, SITES))

    g = [jnp.where(lane < 64, total(n, 0), total(n, 1)) for n in range(9)]
    g00, g01r, g01i, g11, g02r, g02i, g12r, g12i, g22 = g
    ib = 1.0 / (g00 + epsilon)
    kr = (g01r - mass_shift * epsilon) * ib
    ki = g01i * ib
    hr = kr + mass_shift
    hi = ki
    kk = kr * kr + ki * ki
    wp = (g11 - 2.0 * (kr * g01r + ki * g01i) + kk * g00) * ib
    n1 = wp + epsilon
    in1 = 1.0 / n1
    er = epsilon * hr * ib
    ei = epsilon * hi * ib
    tr = (g02r - (kr * g01r - ki * g01i)) * ib
    ti = (g02i - (kr * g01i + ki * g01r)) * ib
    sr = mass_shift * er + tr
    si = mass_shift * ei + ti
    both = ib * in1
    ur = (g12r - kr * g11 - (kr * g02r + ki * g02i) + kk * g01r) * both
    ui = (g12i - ki * g11 - (kr * g02i - ki * g02r) + kk * g01i) * both
    pr = ur - mass_shift * epsilon * in1
    pi = ui
    h11r = pr + mass_shift
    h11i = pi
    q2 = (g22 - 2.0 * (kr * g12r + ki * g12i) + kk * g11) * both
    cross = sr * (pr * er - pi * ei) + si * (pr * ei + pi * er)
    n2 = (
        q2
        + (sr * sr + si * si) * in1 * (g00 * ib)
        + (pr * pr + pi * pi) * (wp * in1)
        - 2.0 * (sr * tr + si * ti) * in1
        - 2.0 * (pr * ur + pi * ui)
        + 2.0 * cross * in1
        + epsilon
    )
    mr = hr * h11r - hi * h11i - sr
    mi = hr * h11i + hi * h11r - si
    idet = 1.0 / (mr * mr + mi * mi + n2 * (hr * hr + hi * hi + n1))
    x1r = -mr * idet
    x1i = mi * idet
    fr = h11r + kr
    fi = h11i + ki
    x0r = (fr * mr + fi * mi + hr * n2) * idet
    x0i = (fi * mr - fr * mi - hi * n2) * idet

    d0r = 1.0 - mass_shift * x0r
    d0i = -mass_shift * x0i
    d1r = mass_shift * x1r + x0r
    d1i = mass_shift * x1i + x0i
    for n in range(SITES // 8):
        rows = slice(8 * n, 8 * n + 8)
        a, ia = start[rows, :], upright[0, rows, :]
        b, ib_, c, ic = (upright[k, rows, :] for k in range(1, 5))
        both_ref[0, rows, :] = x0r * a + x0i * ia + x1r * b + x1i * ib_
        both_ref[1, rows, :] = (
            d0r * a + d0i * ia - (d1r * b + d1i * ib_) - (x1r * c + x1i * ic)
        )
    pltpu.make_async_copy(halo_in, halo_in, halo_send).wait()
    pltpu.make_async_copy(whole, whole, sum_send).wait()


def finish(both_ref, sol_ref, res_ref, sems):
    copies = [
        pltpu.make_async_copy(both_ref.at[n], out, sems.at[n])
        for n, out in enumerate((sol_ref, res_ref))
    ]
    for copy in copies:
        copy.start()
    for copy in copies:
        copy.wait()


def shards(sizes, right_side, link_blocks):
    others = offsets_of(sizes)[-1]
    f32 = jnp.float32
    both = pl.pallas_call(
        functools.partial(kernel, sizes),
        out_shape=jax.ShapeDtypeStruct((2, SITES, VEC), f32),
        in_specs=[pl.BlockSpec(memory_space=pl.ANY)] * 2,
        out_specs=pl.BlockSpec(memory_space=pltpu.VMEM),
        scratch_shapes=[
            pltpu.VMEM((9, 2, DOF, DOF, SITES), f32),
            pltpu.VMEM((SITES, VEC), f32),
            pltpu.VMEM((3, VEC, SITES), f32),
            pltpu.VMEM((12, RHS, 3, DOF, SITES), f32),
            pltpu.VMEM((DOF, 6, 8, SITES), f32),
            pltpu.VMEM((3, 2, DOF, DOF, SITES), f32),
            pltpu.VMEM((3, DOF, DOF, SITES), f32),
            pltpu.VMEM((5, SITES, VEC), f32),
            pltpu.VMEM((2, RHS, 2, 32, SITES), f32),
            pltpu.VMEM((2, RHS, 2, 8, SITES), f32),
            pltpu.VMEM((2, RHS, 208, SITES), f32),
            pltpu.VMEM((1, SITES), f32),
            pltpu.VMEM((len(others), SITES), f32),
            pltpu.SemaphoreType.DMA((len(LOADS),)),
            pltpu.SemaphoreType.DMA,
            pltpu.SemaphoreType.DMA,
            pltpu.SemaphoreType.DMA((2 * RHS,)),
            pltpu.SemaphoreType.DMA((2 * RHS,)),
            pltpu.SemaphoreType.DMA((2 * RHS,)),
            pltpu.SemaphoreType.DMA,
            pltpu.SemaphoreType.DMA,
            pltpu.SemaphoreType.REGULAR,
            pltpu.SemaphoreType.REGULAR,
            pltpu.SemaphoreType.REGULAR,
        ],
        compiler_params=pltpu.CompilerParams(
            collective_id=0, has_side_effects=True, vmem_limit_bytes=54000 * 1024
        ),
    )(
        pltpu.with_memory_space_constraint(right_side.reshape(SITES, VEC), pltpu.HBM),
        pltpu.with_memory_space_constraint(link_blocks.reshape(9, 2, DOF, DOF, SITES), pltpu.HBM),
    )
    sol, res = pl.pallas_call(
        finish,
        out_shape=(jax.ShapeDtypeStruct((SITES, VEC), f32),) * 2,
        in_specs=[pl.BlockSpec(memory_space=pltpu.VMEM)],
        out_specs=(pl.BlockSpec(memory_space=pl.ANY),) * 2,
        scratch_shapes=[pltpu.SemaphoreType.DMA((2,))],
        compiler_params=pltpu.CompilerParams(vmem_limit_bytes=4 * 1024 * 1024),
    )(both)
    return sol.reshape(right_side.shape), res.reshape(right_side.shape)


def solution(mesh):
    sizes = tuple(mesh.shape[name] for name in AXES)
    spec = P("xy", "gz", "ta", None, None)
    return jax.shard_map(
        functools.partial(shards, sizes),
        mesh=mesh,
        in_specs=(spec, P("xy", "gz", "ta", None, None, None, None, None)),
        out_specs=(spec, spec),
        check_vma=False,
    )
```
